256 devices in a mesh: frames: 16 (over x, y), pix: 16 (over z, core).
Axes of the slice: x: 4, y: 4, z: 8, core: 2. Of those that a mesh axis runs over, the one named last changes fastest.
Arguments:
- intensity: bfloat16 [512, 1048576], P('frames', 'pix'), may hold values from -6 to 6
- chi_bin: int32 [1048576], P('pix'), may hold values from 0 to 255
- split: float32 [1048576], P('pix'), may hold values from 0 to 1
- mask: int32 [1048576], P('pix'), may hold values 0 or 1
- tile_row: int32 [8192], P('pix'), may hold values from 0 to 255
Outputs:
- correlation: float32 [256, 2, 128, 256], P('frames', None, 'pix')
The draws below stay inside these ranges and needn't reach their ends.
All inputs are finite; a program needn't handle non-finite values. No bound on the sum of `mask` on one device may be relied on, other than what follows from the above.
Results may differ from the reference program's by a relative error of at most 0.0027.
Values sent between devices are 32-bit elements; how exact they have to be, the bound alone decides.
A program may use at most 128 MiB of HBM per device.

```python
import math
import jax
import jax.numpy as jnp
from jax import lax

NQ = 256
NCHI = 256
NH = 128
FRAMES = 512
PIX = 1048576
TILES = 8192


def draw_tile_row(key, part):
    base_key = jax.random.fold_in(key, 4243)
    order_key, rows_key, pick_key = jax.random.split(base_key, 3)
    cycle_order = jax.random.permutation(order_key, NQ).astype(jnp.int32)
    slots = jax.random.randint(rows_key, (TILES,), 0, NQ - 8).astype(jnp.int32)
    lonely = jax.random.permutation(pick_key, TILES)[:4].astype(jnp.int32)
    slots = slots.at[lonely].set((NQ - 4 + jnp.arange(4)).astype(jnp.int32))
    return cycle_order[slots].astype(jnp.int32)


def plant(result, key, smallest, largest):
    longest = result.shape.index(max(result.shape))
    spots = []
    for shift in (0, 1):
        where = [jax.random.randint(jax.random.fold_in(key, axis), (), 0, length) for axis, length in enumerate(result.shape)]
        where[longest] = (where[longest] + shift) % result.shape[longest]
        spots.append(tuple(where))
    return result.at[spots[0]].set(smallest).at[spots[1]].set(largest)


def shard_levels(own_key, shape, cuts, least, high):
    def one(position, shards_of):
        heights = jax.random.uniform(jax.random.fold_in(jax.random.fold_in(own_key, 6), position), (shards_of,), jnp.float32, least / len(cuts), high / len(cuts))
        return jnp.repeat(jnp.exp(heights), shape[position] // shards_of).reshape((-1,) + (1,) * (len(shape) - position - 1))

    factor_of = one(*cuts[0])
    for cut in cuts[1:]:
        factor_of = factor_of * one(*cut)
    return factor_of


def gaussian(stream_key, dims, scale, reach, cuts=(), kind=jnp.bfloat16):
    drawn = jax.random.normal(stream_key, dims, jnp.float32) * scale
    if len(cuts) > 0:
        drawn = shard_levels(stream_key, dims, cuts, -0.22, 0.18) * drawn
    return jnp.clip(drawn, min=-reach, max=reach).astype(kind)


def setup_inputs(seed: int = 0) -> dict:
    streams_of = jax.random.split(jax.random.key(seed), 6)
    intensity = gaussian(streams_of[0], (FRAMES, PIX), 1.0, 6.0, ((0, 16), (1, 16)))
    chi_bin = plant(jax.random.randint(streams_of[1], (PIX,), 0, NCHI), jax.random.fold_in(streams_of[1], 1), 0, NCHI - 1).astype(jnp.int32)
    split = jnp.clip(1.0 * jax.random.uniform(streams_of[2], (PIX,), jnp.float32) ** shard_levels(streams_of[2], (PIX,), ((0, 16),), -0.2, 0.2), 0.0, 1.0)
    mask = plant((jax.random.randint(streams_of[3], (PIX,), 0, 8) < 7).astype(jnp.int32), jax.random.fold_in(streams_of[3], 1), 0, 1)
    tile_row = draw_tile_row(jax.random.fold_in(streams_of[5], 71), 0)
    return dict(intensity=intensity, chi_bin=chi_bin, split=split, mask=mask, tile_row=tile_row)


def fourier_table():
    harmonic = lax.iota(jnp.int32, NH)[:, None]
    column = lax.iota(jnp.int32, NCHI)[None, :]
    phases = (harmonic * column % NCHI).astype(jnp.float32) * (2.0 * math.pi / NCHI)
    factor = 1.0 / math.sqrt(NCHI)
    return jnp.stack([jnp.cos(phases) * factor, -jnp.sin(phases) * factor], 0)

def reference(intensity, chi_bin, split, mask, tile_row):
    usable = mask.astype(jnp.float32)
    near_weight = lax.optimization_barrier((usable * split).astype(jnp.bfloat16)).astype(jnp.float32)
    far_weight = lax.optimization_barrier((usable * (1.0 - split)).astype(jnp.bfloat16)).astype(jnp.float32)
    tile_rows = jnp.repeat(tile_row, 128).astype(jnp.int32)
    near_bins = (tile_rows * NCHI + chi_bin).astype(jnp.int32)
    far_bins = (tile_rows * NCHI + (chi_bin + 1) % NCHI).astype(jnp.int32)
    bins_total = NQ * NCHI
    counts = jax.ops.segment_sum(near_weight, near_bins, bins_total) + jax.ops.segment_sum(far_weight, far_bins, bins_total)

    def bin_frame(frame):
        values = frame.astype(jnp.float32)
        return jax.ops.segment_sum(values * near_weight, near_bins, bins_total) + jax.ops.segment_sum(values * far_weight, far_bins, bins_total)
    sums = lax.map(bin_frame, intensity)
    normed = (sums / jnp.maximum(counts, 1.0)).reshape(FRAMES, NQ, NCHI)
    spectra = jnp.einsum('fqc,rnc->frnq', normed, fourier_table(), precision=lax.Precision.HIGHEST)
    real_part = spectra[:, 0]
    imag_part = spectra[:, 1]
    high = lax.Precision.HIGHEST
    real_corr = jnp.einsum('fnq,fnp->qnp', real_part, real_part, precision=high) + jnp.einsum('fnq,fnp->qnp', imag_part, imag_part, precision=high)
    imag_corr = jnp.einsum('fnq,fnp->qnp', imag_part, real_part, precision=high) - jnp.einsum('fnq,fnp->qnp', real_part, imag_part, precision=high)
    return jnp.stack([real_corr, imag_corr], 1) / math.sqrt(FRAMES)
```

```python
import math

import jax
import jax.numpy as jnp
from jax import lax
from jax.experimental import pallas as pl
from jax.experimental.pallas import tpu as pltpu
from jax.sharding import PartitionSpec as P

NQ = 256
NCHI = 256
NH = 128
ROWS = 40
TILE_BLOCK = 128
GROUP = 16


def bin_kernel(tiles_block, rows_ref, x_ref, chi_ref, split_ref, mask_ref, cake_ref, acc, vals, sem):
    step = pl.program_id(0)
    frames = x_ref.shape[0]
    bf = jnp.bfloat16

    @pl.when(step == 0)
    def _():
        acc[...] = jnp.zeros_like(acc)
        vals[...] = jnp.zeros_like(vals)

    zero = jnp.zeros((), bf)
    columns = lax.broadcasted_iota(jnp.int32, (NCHI, 128), 0).astype(jnp.float32).astype(bf)
    row = lax.broadcasted_iota(jnp.int32, (16, 256), 0)
    lane = lax.broadcasted_iota(jnp.int32, (16, 256), 1)
    ones = jnp.where(((row == 0) & (lane < 128)) | ((row == 8) & (lane >= 128)), 1.0, 0.0).astype(bf)
    blank = jnp.zeros((frames, 128), bf)

    def weights_of(t):
        chi = chi_ref[pl.ds(t, 1), :]
        usable = mask_ref[pl.ds(t, 1), :].astype(jnp.float32)
        split = split_ref[pl.ds(t, 1), :]
        near = (usable * split).astype(bf)
        far = (usable * (1.0 - split)).astype(bf)
        here = chi.astype(jnp.float32).astype(bf)
        after = ((chi + 1) & (NCHI - 1)).astype(jnp.float32).astype(bf)
        return jnp.where(columns == here, near, jnp.where(columns == after, far, zero))

    def group(g, carry):
        slot = lax.rem(g, 2)
        for u in range(0, GROUP, 2):
            t = g * GROUP + u
            weights = jnp.concatenate([weights_of(t), weights_of(t + 1)], axis=1)
            a = x_ref[:, pl.ds(pl.multiple_of(t * 128, 128), 128)]
            b = x_ref[:, pl.ds(pl.multiple_of(t * 128 + 128, 128), 128)]
            left = jnp.concatenate(
                [jnp.concatenate([a, blank], 1), jnp.concatenate([blank, b], 1), ones], axis=0
            )
            value = lax.dot_general(
                left, weights, (((1,), (1,)), ((), ())), preferred_element_type=jnp.float32
            )
            vals[slot, u, :frames] = value[:frames]
            vals[slot, u, frames:] = value[2 * frames:2 * frames + 8]
            vals[slot, u + 1, :frames] = value[frames:2 * frames]
            vals[slot, u + 1, frames:] = value[2 * frames + 8:]
        before = jnp.maximum(step * tiles_block + (g - 1) * GROUP, 0)
        for u in range(GROUP):
            q = rows_ref[before + u]
            acc[q] = acc[q] + vals[1 - slot, u]
        return carry

    groups = tiles_block // GROUP
    lax.fori_loop(0, groups, group, 0)

    @pl.when(step == pl.num_programs(0) - 1)
    def _():
        for u in range(GROUP):
            q = rows_ref[(step + 1) * tiles_block - GROUP + u]
            acc[q] = acc[q] + vals[(groups - 1) % 2, u]
        copy = pltpu.make_async_copy(acc, cake_ref, sem)
        copy.start()
        copy.wait()


def binned(intensity, chi_bin, split, mask, tile_row):
    frames = intensity.shape[0]
    tiles = tile_row.shape[0]
    block = TILE_BLOCK
    flat = pl.BlockSpec((block, 128), lambda i, rows: (i, 0))
    return pl.pallas_call(
        lambda *refs: bin_kernel(block, *refs),
        out_shape=jax.ShapeDtypeStruct((NQ, ROWS, NCHI), jnp.float32),
        grid_spec=pltpu.PrefetchScalarGridSpec(
            num_scalar_prefetch=1,
            grid=(tiles // block,),
            in_specs=[pl.BlockSpec((frames, block * 128), lambda i, rows: (0, i)), flat, flat, flat],
            out_specs=pl.BlockSpec(memory_space=pl.ANY),
            scratch_shapes=[
                pltpu.VMEM((NQ, ROWS, NCHI), jnp.float32),
                pltpu.VMEM((2, GROUP, ROWS, NCHI), jnp.float32),
                pltpu.SemaphoreType.DMA,
            ],
        ),
        compiler_params=pltpu.CompilerParams(
            dimension_semantics=("arbitrary",), vmem_limit_bytes=40 << 20
        ),
        name="binning",
    )(tile_row, intensity, *(a.reshape(tiles, 128) for a in (chi_bin, split, mask)))


def fourier_table():
    harmonic = lax.iota(jnp.int32, NH)[:, None]
    column = lax.iota(jnp.int32, NCHI)[None, :]
    phases = (harmonic * column % NCHI).astype(jnp.float32) * (2.0 * math.pi / NCHI)
    factor = 1.0 / math.sqrt(NCHI)
    return jnp.stack([jnp.cos(phases) * factor, -jnp.sin(phases) * factor], 0)


def body(intensity, chi_bin, split, mask, tile_row):
    frames_dev = intensity.shape[0]
    high = lax.Precision.HIGHEST
    cake = binned(intensity, chi_bin, split, mask, tile_row)[:, :frames_dev + 1]
    block = lax.psum_scatter(cake, "pix", scatter_dimension=0, tiled=True)
    normed = block[:, :frames_dev] / jnp.maximum(block[:, frames_dev:], 1.0)
    local_spectra = jnp.einsum("qfc,rnc->frnq", normed, fourier_table(), precision=high)
    spectra = lax.all_to_all(local_spectra, "pix", split_axis=2, concat_axis=3, tiled=True)
    frame_scale = 1.0 / math.sqrt(frames_dev * lax.axis_size("frames"))
    real_part = spectra[:, 0]
    imag_part = spectra[:, 1]
    real_corr = jnp.einsum("fnq,fnp->qnp", real_part, real_part, precision=high) + jnp.einsum(
        "fnq,fnp->qnp", imag_part, imag_part, precision=high
    )
    imag_corr = jnp.einsum("fnq,fnp->qnp", imag_part, real_part, precision=high) - jnp.einsum(
        "fnq,fnp->qnp", real_part, imag_part, precision=high
    )
    return lax.psum_scatter(
        jnp.stack([real_corr, imag_corr], 1) * frame_scale,
        "frames",
        scatter_dimension=0,
        tiled=True,
    )


def solution(mesh):
    in_specs = (P("frames", "pix"), P("pix"), P("pix"), P("pix"), P("pix"))
    out_specs = P("frames", None, "pix", None)
    return jax.shard_map(body, mesh=mesh, in_specs=in_specs, out_specs=out_specs, check_vma=False)
```

```python
import math

import jax
import jax.numpy as jnp
import numpy as np
from jax import lax
from jax.experimental import pallas as pl
from jax.experimental.pallas import tpu as pltpu
from jax.sharding import PartitionSpec as P

NQ = 256
NCHI = 256
NH = 128
ROWS = 40
TILE_BLOCK = 128
GROUP = 16
MESH = pl.DeviceIdType.MESH
SUBS = 8
PARTS = 4
TN = (((0,), (0,)), ((), ()))
NT = (((1,), (1,)), ((), ()))


def bin_kernel(tiles_block, rows_ref, x_ref, chi_ref, split_ref, mask_ref, cake_ref, count_ref, acc, vals, sem):
    step = pl.program_id(0)
    frames = x_ref.shape[0]
    bf = jnp.bfloat16

    @pl.when(step == 0)
    def _():
        acc[...] = jnp.zeros_like(acc)
        vals[...] = jnp.zeros_like(vals)

    zero = jnp.zeros((), bf)
    columns = lax.broadcasted_iota(jnp.int32, (NCHI, 128), 0).astype(jnp.float32).astype(bf)
    row = lax.broadcasted_iota(jnp.int32, (16, 256), 0)
    lane = lax.broadcasted_iota(jnp.int32, (16, 256), 1)
    ones = jnp.where(((row == 0) & (lane < 128)) | ((row == 8) & (lane >= 128)), 1.0, 0.0).astype(bf)
    blank = jnp.zeros((frames, 128), bf)

    def weights_of(t):
        chi = chi_ref[pl.ds(t, 1), :]
        usable = mask_ref[pl.ds(t, 1), :].astype(jnp.float32)
        split = split_ref[pl.ds(t, 1), :]
        near = (usable * split).astype(bf)
        far = (usable * (1.0 - split)).astype(bf)
        here = chi.astype(jnp.float32).astype(bf)
        after = ((chi + 1) & (NCHI - 1)).astype(jnp.float32).astype(bf)
        return jnp.where(columns == here, near, jnp.where(columns == after, far, zero))

    def group(g, carry):
        slot = lax.rem(g, 2)
        for u in range(0, GROUP, 2):
            t = g * GROUP + u
            weights = jnp.concatenate([weights_of(t), weights_of(t + 1)], axis=1)
            a = x_ref[:, pl.ds(pl.multiple_of(t * 128, 128), 128)]
            b = x_ref[:, pl.ds(pl.multiple_of(t * 128 + 128, 128), 128)]
            left = jnp.concatenate(
                [jnp.concatenate([a, blank], 1), jnp.concatenate([blank, b], 1), ones], axis=0
            )
            value = lax.dot_general(
                left, weights, (((1,), (1,)), ((), ())), preferred_element_type=jnp.float32
            )
            vals[slot, u, :frames] = value[:frames]
            vals[slot, u, frames:] = value[2 * frames:2 * frames + 8]
            vals[slot, u + 1, :frames] = value[frames:2 * frames]
            vals[slot, u + 1, frames:] = value[2 * frames + 8:]
        before = jnp.maximum(step * tiles_block + (g - 1) * GROUP, 0)
        for u in range(GROUP):
            q = rows_ref[before + u]
            acc[q] = acc[q] + vals[1 - slot, u]
        return carry

    groups = tiles_block // GROUP
    lax.fori_loop(0, groups, group, 0)

    @pl.when(step == pl.num_programs(0) - 1)
    def _():
        for u in range(GROUP):
            q = rows_ref[(step + 1) * tiles_block - GROUP + u]
            acc[q] = acc[q] + vals[(groups - 1) % 2, u]
        copy = pltpu.make_async_copy(acc.at[:, pl.ds(0, frames), :], cake_ref, sem)
        copy.start()

        def rows_of(b, carry):
            at = pl.ds(pl.multiple_of(b * 8, 8), 8)
            count_ref[at, :] = acc[at, frames, :]
            return carry

        lax.fori_loop(0, NQ // 8, rows_of, 0)
        copy.wait()


def binned(intensity, chi_bin, split, mask, tile_row):
    frames = intensity.shape[0]
    tiles = tile_row.shape[0]
    block = TILE_BLOCK
    flat = pl.BlockSpec((block, 128), lambda i, rows: (i, 0))
    return pl.pallas_call(
        lambda *refs: bin_kernel(block, *refs),
        out_shape=(
            jax.ShapeDtypeStruct((NQ, frames, NCHI), jnp.float32),
            jax.ShapeDtypeStruct((NQ, NCHI), jnp.float32),
        ),
        grid_spec=pltpu.PrefetchScalarGridSpec(
            num_scalar_prefetch=1,
            grid=(tiles // block,),
            in_specs=[pl.BlockSpec((frames, block * 128), lambda i, rows: (0, i)), flat, flat, flat],
            out_specs=(
                pl.BlockSpec(memory_space=pl.ANY),
                pl.BlockSpec((NQ, NCHI), lambda i, rows: (0, 0)),
            ),
            scratch_shapes=[
                pltpu.VMEM((NQ, ROWS, NCHI), jnp.float32),
                pltpu.VMEM((2, GROUP, ROWS, NCHI), jnp.float32),
                pltpu.SemaphoreType.DMA,
            ],
        ),
        compiler_params=pltpu.CompilerParams(
            dimension_semantics=("arbitrary",), vmem_limit_bytes=40 << 20
        ),
        name="binning",
    )(tile_row, intensity, *(a.reshape(tiles, 128) for a in (chi_bin, split, mask)))


def halves(x):
    high = x.astype(jnp.bfloat16)
    return high, (x - high.astype(jnp.float32)).astype(jnp.bfloat16)


def dot(a, b, dims):
    return lax.dot_general(a, b, dims, preferred_element_type=jnp.float32)


def link_kernel(
    chips, groups, cake_ref, count_ref, high_ref, low_ref, out_ref,
    own, other, high_in, low_in, spectra, arrived, c1, c2, inverse,
    sent, mine, theirs, corr, landed,
    own_sem, pair_send, pair_recv, c1_send, c1_recv, c2_send, c2_recv,
    ring_send, ring_recv, z_send, z_recv, swap_send, swap_recv, out_send, out_recv, self_sem,
):
    fg = lax.axis_index("frames")
    p = lax.axis_index("pix")
    z = p // 2
    core = p % 2
    devices = 2 * chips
    frames = cake_ref.shape[1]
    half = NQ // 2
    part = half // PARTS
    per = frames // SUBS
    rows = 2 * NH // chips
    lanes = per * half

    def own_copy(i):
        at = pl.ds(pl.multiple_of(i * part, 8), part)
        src = pl.ds(pl.multiple_of(core * half + i * part, 8), part)
        return pltpu.make_async_copy(cake_ref.at[src], own.at[at], own_sem.at[i])

    for i in range(PARTS):
        own_copy(i).start()

    barrier = pltpu.get_barrier_semaphore()

    def greet(d, carry):
        pl.semaphore_signal(barrier, inc=1, device_id=(fg, (p + d) % devices), device_id_type=MESH)
        return carry

    def greet_frames(d, carry):
        there = (fg + d) % groups
        pl.semaphore_signal(barrier, inc=1, device_id=(there, p), device_id_type=MESH)
        pl.semaphore_signal(barrier, inc=1, device_id=(there, 2 * z + 1 - core), device_id_type=MESH)
        return carry

    lax.fori_loop(1, devices, greet, 0)
    lax.fori_loop(1, groups, greet_frames, 0)
    pl.semaphore_wait(barrier, devices - 1 + 2 * (groups - 1))

    def c1_copy(d):
        to = (p + d) % devices
        src = pl.ds(pl.multiple_of((to % 2) * half + fg * 8, 8), 8)
        return pltpu.make_async_remote_copy(
            src_ref=count_ref.at[src, :], dst_ref=c1.at[p], send_sem=c1_send.at[d], recv_sem=c1_recv.at[d],
            device_id=(fg, to), device_id_type=MESH,
        )

    def c1_start(d, carry):
        c1_copy(d).start()
        return carry

    lax.fori_loop(1, devices, c1_start, 0)

    def pair_copy(i):
        at = pl.ds(pl.multiple_of(i * part, 8), part)
        src = pl.ds(pl.multiple_of((1 - core) * half + i * part, 8), part)
        return pltpu.make_async_remote_copy(
            src_ref=cake_ref.at[src], dst_ref=other.at[at], send_sem=pair_send.at[i], recv_sem=pair_recv.at[i],
            device_id=(fg, 2 * z + 1 - core), device_id_type=MESH,
        )

    for i in range(PARTS):
        pair_copy(i).start()

    c1[p] = count_ref[pl.ds(pl.multiple_of(core * half + fg * 8, 8), 8), :]

    def c1_wait(d, carry):
        c1_copy(d).wait()
        return carry

    lax.fori_loop(1, devices, c1_wait, 0)
    total = c1[0]
    for i in range(1, devices):
        total = total + c1[i]
    here = pl.ds(pl.multiple_of(fg * 8, 8), 8)
    c2[here, :] = total

    def c2_copy(d):
        return pltpu.make_async_remote_copy(
            src_ref=c2.at[here, :], dst_ref=c2.at[here, :], send_sem=c2_send.at[d], recv_sem=c2_recv.at[d],
            device_id=((fg + d) % groups, p), device_id_type=MESH,
        )

    def c2_landing(d):
        at = pl.ds(pl.multiple_of((fg + groups - d) % groups * 8, 8), 8)
        return pltpu.make_async_remote_copy(
            src_ref=c2.at[here, :], dst_ref=c2.at[at, :], send_sem=c2_send.at[d], recv_sem=c2_recv.at[d],
            device_id=((fg + d) % groups, p), device_id_type=MESH,
        )

    def c2_start(d, carry):
        c2_copy(d).start()
        return carry

    def c2_wait(d, carry):
        c2_copy(d).wait_send()
        c2_landing(d).wait_recv()
        return carry

    lax.fori_loop(1, groups, c2_start, 0)
    lax.fori_loop(1, groups, c2_wait, 0)
    inverse[...] = 1.0 / jnp.maximum(c2[...], 1.0)

    for i in range(PARTS):
        own_copy(i).wait()
        pair_copy(i).wait()

    def normalise(n, carry):
        b = n // (frames // 8)
        f = n % (frames // 8)
        qs = pl.ds(pl.multiple_of(b * 16, 16), 16)
        fs = pl.ds(pl.multiple_of(f * 8, 8), 8)
        both = jnp.swapaxes(own[qs, fs, :] + other[qs, fs, :], 0, 1) * inverse[qs, :][None]
        h, l = halves(both)
        high_in[fs, qs, :] = h
        low_in[fs, qs, :] = l
        return carry

    lax.fori_loop(0, half // 16 * (frames // 8), normalise, 0)

    def ring_copy(k, s):
        sign = 1 - 2 * (k % 2)
        block = (z - sign * (1 + s) + 2 * chips) % chips
        at = pl.ds(pl.multiple_of(block * rows, 8), rows)
        return pltpu.make_async_remote_copy(
            src_ref=spectra.at[k, at, :], dst_ref=arrived.at[k, s],
            send_sem=ring_send.at[k, s], recv_sem=ring_recv.at[k, s],
            device_id=(fg, 2 * ((z + sign + chips) % chips) + core), device_id_type=MESH,
        )

    def transform(k, carry):
        for t in range(0, per, 2):
            fs = pl.ds(k * per + t, 2)
            h = high_in[fs].reshape(2 * half, NCHI)
            l = low_in[fs].reshape(2 * half, NCHI)
            spectra[k, :, t * half:(t + 2) * half] = (
                dot(high_ref[...], h, NT) + dot(high_ref[...], l, NT) + dot(low_ref[...], h, NT)
            )
        ring_copy(k, 0).start()
        return carry

    lax.fori_loop(0, SUBS, transform, 0)

    def take(k, s):
        sign = 1 - 2 * (k % 2)
        block = (z - sign * (2 + s) + 2 * chips) % chips
        at = pl.ds(pl.multiple_of(block * rows, 8), rows)
        ring_copy(k, s).wait_recv()
        spectra[k, at, :] = spectra[k, at, :] + arrived[k, s]

    def ring_step(n, carry):
        s = n // SUBS
        k = n % SUBS
        take(k, s)
        ring_copy(k, s + 1).start()
        return carry

    lax.fori_loop(0, (chips - 2) * SUBS, ring_step, 0)

    def z_copy(g, d):
        to = (fg + d) % groups
        fs = pl.ds(pl.multiple_of(g * 8, 8), 8)
        return pltpu.make_async_remote_copy(
            src_ref=sent.at[pl.ds(2 * to, 2), fs, :], dst_ref=mine.at[fg, :, fs, :],
            send_sem=z_send.at[g, d], recv_sem=z_recv.at[g, d],
            device_id=(to, p), device_id_type=MESH,
        )

    def z_landing(g, d):
        fs = pl.ds(pl.multiple_of(g * 8, 8), 8)
        return pltpu.make_async_remote_copy(
            src_ref=sent.at[pl.ds(0, 2), fs, :], dst_ref=mine.at[(fg + groups - d) % groups, :, fs, :],
            send_sem=z_send.at[g, d], recv_sem=z_recv.at[g, d],
            device_id=((fg + d) % groups, p), device_id_type=MESH,
        )

    pack = 8 // per

    def finish(g, carry):
        for i in range(pack):
            take(g * pack + i, chips - 2)
        for t in range(rows // 8):
            at = pl.ds(pl.multiple_of(z * rows + t * 8, 8), 8)
            pieces = [
                spectra[g * pack + i, at, f * half:(f + 1) * half] for i in range(pack) for f in range(per)
            ]
            turned = jnp.swapaxes(jnp.stack(pieces, 0), 0, 1)
            sent[t * 8:t * 8 + 8, pl.ds(pl.multiple_of(g * 8, 8), 8), :] = turned

        def z_start(d, carry):
            z_copy(g, d).start()
            return carry

        lax.fori_loop(1, groups, z_start, 0)
        return carry

    lax.fori_loop(0, frames // 8, finish, 0)
    mine[fg] = sent[pl.ds(2 * fg, 2)]

    def z_wait(n, carry):
        g = n // (groups - 1)
        d = 1 + n % (groups - 1)
        z_landing(g, d).wait_recv()
        return carry

    lax.fori_loop(0, frames // 8 * (groups - 1), z_wait, 0)

    swap = pltpu.make_async_remote_copy(
        src_ref=mine, dst_ref=theirs, send_sem=swap_send, recv_sem=swap_recv,
        device_id=(fg, 2 * z + 1 - core), device_id_type=MESH,
    )
    swap.start()
    total_frames = groups * frames
    scale = 1.0 / math.sqrt(total_frames)

    real = mine[:, 0].reshape(total_frames, half)
    imag = mine[:, 1].reshape(total_frames, half)
    real_high, real_low = halves(real)
    imag_high, imag_low = halves(imag)

    def left_of(r, i):
        return jnp.concatenate([jnp.concatenate([r, i], 1), jnp.concatenate([i, -r], 1)], 0)

    left_high = left_of(real_high, imag_high)
    left_low = left_of(real_low, imag_low)

    def product(right_high, right_low):
        return (
            dot(left_high, right_high, TN) + dot(left_high, right_low, TN) + dot(left_low, right_high, TN)
        ) * scale

    near = product(
        jnp.concatenate([real_high, imag_high], 0), jnp.concatenate([real_low, imag_low], 0)
    )
    corr[core] = near.reshape(2, half, half)
    swap.wait()
    far_high, far_low = halves(
        jnp.concatenate(
            [theirs[:, 0].reshape(total_frames, half), theirs[:, 1].reshape(total_frames, half)], 0
        )
    )
    corr[1 - core] = product(far_high, far_low).reshape(2, half, half)

    block = NQ // groups
    blocks = groups // 2
    owner_core = fg // blocks

    def out_copy(i):
        return pltpu.make_async_remote_copy(
            src_ref=corr.at[:, :, pl.ds(pl.multiple_of(i * block, 8), block), :], dst_ref=landed.at[fg % blocks],
            send_sem=out_send.at[i], recv_sem=out_recv.at[fg % blocks],
            device_id=(core * blocks + i, 2 * z + owner_core), device_id_type=MESH,
        )

    def out_landing(n):
        return pltpu.make_async_remote_copy(
            src_ref=corr.at[:, :, pl.ds(0, block), :], dst_ref=landed.at[n],
            send_sem=out_send.at[n], recv_sem=out_recv.at[n],
            device_id=(core * blocks + n, 2 * z + owner_core), device_id_type=MESH,
        )

    def out_start(i, carry):
        @pl.when(core * blocks + i != fg)
        def _():
            out_copy(i).start()

        return carry

    lax.fori_loop(0, blocks, out_start, 0)

    @pl.when(owner_core == core)
    def _():
        i = fg % blocks
        keep = pltpu.make_async_copy(
            corr.at[:, :, pl.ds(pl.multiple_of(i * block, 8), block), :], landed.at[i], self_sem
        )
        keep.start()
        keep.wait()

    def out_wait(n, carry):
        @pl.when(core * blocks + n != fg)
        def _():
            out_landing(n).wait_recv()
            out_copy(n).wait_send()

        return carry

    lax.fori_loop(0, blocks, out_wait, 0)
    out_ref[...] = landed[...]

    def ring_done(n, carry):
        ring_copy(n % SUBS, n // SUBS).wait_send()
        return carry

    lax.fori_loop(0, (chips - 1) * SUBS, ring_done, 0)

    def z_done(n, carry):
        z_copy(n // (groups - 1), 1 + n % (groups - 1)).wait_send()
        return carry

    lax.fori_loop(0, frames // 8 * (groups - 1), z_done, 0)


def linked(cake, counts, chips, groups):
    frames = cake.shape[1]
    devices = 2 * chips
    half = NQ // 2
    part = half // PARTS
    per = frames // SUBS
    rows = 2 * NH // chips
    block = NQ // groups
    blocks = groups // 2
    high, low = fourier_table()
    f32, bf = jnp.float32, jnp.bfloat16
    dma = pltpu.SemaphoreType.DMA
    vmem = pl.BlockSpec(memory_space=pltpu.VMEM)
    return pl.pallas_call(
        lambda *refs: link_kernel(chips, groups, *refs),
        out_shape=jax.ShapeDtypeStruct((blocks, 2, 2, block, half), f32),
        in_specs=[pl.BlockSpec(memory_space=pl.ANY), vmem, vmem, vmem],
        out_specs=vmem,
        scratch_shapes=[
            pltpu.VMEM((half, frames, NCHI), f32),
            pltpu.VMEM((half, frames, NCHI), f32),
            pltpu.VMEM((frames, half, NCHI), bf),
            pltpu.VMEM((frames, half, NCHI), bf),
            pltpu.VMEM((SUBS, 2 * NH, per * half), f32),
            pltpu.VMEM((SUBS, chips - 1, rows, per * half), f32),
            pltpu.VMEM((devices, 8, NCHI), f32),
            pltpu.VMEM((half, NCHI), f32),
            pltpu.VMEM((half, NCHI), f32),
            pltpu.VMEM((rows, frames, half), f32),
            pltpu.VMEM((groups, 2, frames, half), f32),
            pltpu.VMEM((groups, 2, frames, half), f32),
            pltpu.VMEM((2, 2, half, half), f32),
            pltpu.VMEM((blocks, 2, 2, block, half), f32),
            dma((PARTS,)), dma((PARTS,)), dma((PARTS,)),
            dma((devices,)), dma((devices,)), dma((groups,)), dma((groups,)),
            dma((SUBS, chips - 1)), dma((SUBS, chips - 1)),
            dma((frames // 8, groups)), dma((frames // 8, groups)),
            dma(()), dma(()), dma((blocks,)), dma((blocks,)), dma(()),
        ],
        compiler_params=pltpu.CompilerParams(
            collective_id=0, has_side_effects=True, vmem_limit_bytes=48 << 20
        ),
        name="links",
    )(cake, counts, jnp.asarray(high), jnp.asarray(low))


def fourier_table():
    harmonic = np.arange(NH)[:, None]
    phases = (harmonic * np.arange(NCHI)[None, :] % NCHI) * (2.0 * math.pi / NCHI)
    table = np.stack([np.cos(phases), -np.sin(phases)], 1) / math.sqrt(NCHI)
    table = table.reshape(2 * NH, NCHI).astype(np.float32)
    high = table.astype(jnp.bfloat16)
    return high, (table - high.astype(np.float32)).astype(jnp.bfloat16)


def solution(mesh):
    groups = mesh.shape["frames"]
    chips = mesh.shape["pix"] // 2

    def body(intensity, chi_bin, split, mask, tile_row):
        cake, counts = binned(intensity, chi_bin, split, mask, tile_row)
        blocks = linked(cake, counts, chips, groups)
        n, h, c, q, r = blocks.shape
        return blocks.transpose(3, 2, 0, 1, 4).reshape(q, c, n, h * r)

    in_specs = (P("frames", "pix"), P("pix"), P("pix"), P("pix"), P("pix"))
    out_specs = P("frames", None, "pix", None)
    return jax.shard_map(body, mesh=mesh, in_specs=in_specs, out_specs=out_specs, check_vma=False)
```

```python
import math

import jax
import jax.numpy as jnp
import numpy as np
from jax import lax
from jax.experimental import pallas as pl
from jax.experimental.pallas import tpu as pltpu
from jax.sharding import PartitionSpec as P

NQ = 256
NCHI = 256
NH = 128
ROWS = 40
TILE_BLOCK = 64
GROUP = 16
BIN_VMEM = 36 << 20
LINK_VMEM = 36 << 20
MESH = pl.DeviceIdType.MESH
SUBS = 8
PARTS = 4
TN = (((0,), (0,)), ((), ()))
NT = (((1,), (1,)), ((), ()))


def bin_kernel(
    rows_any, x_any, chi_any, split_any, mask_any, cake_ref, count_ref,
    rows_ref, x_ref, chi_ref, split_ref, mask_ref, count_acc, vals, rows_sem, sem,
):
    frames = x_ref.shape[0]
    tiles = chi_ref.shape[0]
    blocks = tiles // TILE_BLOCK
    bf = jnp.bfloat16

    def copies(b):
        at = pl.ds(pl.multiple_of(b * TILE_BLOCK, 8), TILE_BLOCK)
        wide = pl.ds(pl.multiple_of(b * TILE_BLOCK * 128, 128), TILE_BLOCK * 128)
        pairs = ((chi_any, chi_ref), (split_any, split_ref), (mask_any, mask_ref))
        flat = [pltpu.make_async_copy(a.at[at, :], r.at[at, :], sem.at[b, n]) for n, (a, r) in enumerate(pairs)]
        return flat + [pltpu.make_async_copy(x_any.at[:, wide], x_ref.at[:, wide], sem.at[b, 3])]

    rows_copy = pltpu.make_async_copy(rows_any, rows_ref, rows_sem)
    rows_copy.start()
    for b in range(blocks):
        for copy in copies(b):
            copy.start()

    def clear(n, carry):
        at = pl.ds(n * 8, 8)
        cake_ref[at] = jnp.zeros((8, frames, NCHI), jnp.float32)
        count_acc[at] = jnp.zeros((8, 8, NCHI), jnp.float32)
        return carry

    lax.fori_loop(0, NQ // 8, clear, 0)
    vals[...] = jnp.zeros_like(vals)

    zero = jnp.zeros((), bf)
    columns = lax.broadcasted_iota(jnp.int32, (NCHI, 128), 0).astype(jnp.float32).astype(bf)
    row = lax.broadcasted_iota(jnp.int32, (16, 256), 0)
    lane = lax.broadcasted_iota(jnp.int32, (16, 256), 1)
    ones = jnp.where(((row == 0) & (lane < 128)) | ((row == 8) & (lane >= 128)), 1.0, 0.0).astype(bf)
    blank = jnp.zeros((frames, 128), bf)

    def weights_of(t):
        chi = chi_ref[pl.ds(t, 1), :]
        usable = mask_ref[pl.ds(t, 1), :].astype(jnp.float32)
        split = split_ref[pl.ds(t, 1), :]
        near = (usable * split).astype(bf)
        far = (usable * (1.0 - split)).astype(bf)
        here = chi.astype(jnp.float32).astype(bf)
        after = ((chi + 1) & (NCHI - 1)).astype(jnp.float32).astype(bf)
        return jnp.where(columns == here, near, jnp.where(columns == after, far, zero))

    def add(first, slot):
        for u in range(GROUP):
            q = rows_ref[first + u]
            cake_ref[q] = cake_ref[q] + vals[slot, u, :frames]
            count_acc[q] = count_acc[q] + vals[slot, u, frames:]

    def group(g, carry):
        slot = lax.rem(g, 2)

        @pl.when(lax.rem(g * GROUP, TILE_BLOCK) == 0)
        def _():
            for copy in copies(g * GROUP // TILE_BLOCK):
                copy.wait()

        for u in range(0, GROUP, 2):
            t = g * GROUP + u
            weights = jnp.concatenate([weights_of(t), weights_of(t + 1)], axis=1)
            a = x_ref[:, pl.ds(pl.multiple_of(t * 128, 128), 128)]
            b = x_ref[:, pl.ds(pl.multiple_of(t * 128 + 128, 128), 128)]
            left = jnp.concatenate(
                [jnp.concatenate([a, blank], 1), jnp.concatenate([blank, b], 1), ones], axis=0
            )
            value = dot(left, weights, NT)
            vals[slot, u, :frames] = value[:frames]
            vals[slot, u, frames:] = value[2 * frames:2 * frames + 8]
            vals[slot, u + 1, :frames] = value[frames:2 * frames]
            vals[slot, u + 1, frames:] = value[2 * frames + 8:]
        add(jnp.maximum((g - 1) * GROUP, 0), 1 - slot)
        return carry

    rows_copy.wait()
    groups = tiles // GROUP
    lax.fori_loop(0, groups, group, 0)
    add(tiles - GROUP, (groups - 1) % 2)

    def rows_of(b, carry):
        at = pl.ds(pl.multiple_of(b * 8, 8), 8)
        count_ref[at, :] = count_acc[at, 0, :]
        return carry

    lax.fori_loop(0, NQ // 8, rows_of, 0)


def stay(a):
    return pltpu.with_memory_space_constraint(a, pltpu.HBM)


def binned(intensity, chi_bin, split, mask, tile_row):
    frames, pixels = intensity.shape
    tiles = tile_row.shape[0]
    vmem = pl.BlockSpec(memory_space=pltpu.VMEM)
    away = pl.BlockSpec(memory_space=pltpu.HBM)
    return pl.pallas_call(
        bin_kernel,
        out_shape=(
            jax.ShapeDtypeStruct((NQ, frames, NCHI), jnp.float32),
            jax.ShapeDtypeStruct((NQ, NCHI), jnp.float32),
        ),
        in_specs=[away, away, away, away, away],
        out_specs=(vmem, vmem),
        scratch_shapes=[
            pltpu.SMEM((tiles,), jnp.int32),
            pltpu.VMEM((frames, pixels), jnp.bfloat16),
            pltpu.VMEM((tiles, 128), jnp.int32),
            pltpu.VMEM((tiles, 128), jnp.float32),
            pltpu.VMEM((tiles, 128), jnp.int32),
            pltpu.VMEM((NQ, 8, NCHI), jnp.float32),
            pltpu.VMEM((2, GROUP, ROWS, NCHI), jnp.float32),
            pltpu.SemaphoreType.DMA,
            pltpu.SemaphoreType.DMA((tiles // TILE_BLOCK, 4)),
        ],
        compiler_params=pltpu.CompilerParams(vmem_limit_bytes=BIN_VMEM),
        name="binning",
    )(*(stay(a) for a in (tile_row, intensity, *(a.reshape(tiles, 128) for a in (chi_bin, split, mask)))))


def halves(x):
    high = x.astype(jnp.bfloat16)
    return high, (x - high.astype(jnp.float32)).astype(jnp.bfloat16)


def dot(a, b, dims):
    return lax.dot_general(a, b, dims, preferred_element_type=jnp.float32)


def link_kernel(
    chips, groups, cake_ref, count_ref, high_any, low_any, out_ref,
    high_ref, low_ref, other, high_in, low_in, spectra, arrived, c1, c2, inverse,
    sent, mine, theirs, corr, landed,
    table_sem, pair_send, pair_recv, c1_send, c1_recv, c2_send, c2_recv,
    ring_send, ring_recv, z_send, z_recv, swap_send, swap_recv, out_send, out_recv, self_sem,
):
    fg = lax.axis_index("frames")
    p = lax.axis_index("pix")
    z = p // 2
    core = p % 2
    devices = 2 * chips
    frames = cake_ref.shape[1]
    half = NQ // 2
    part = half // PARTS
    per = frames // SUBS
    rows = 2 * NH // chips
    lanes = per * half

    tables = [
        pltpu.make_async_copy(high_any, high_ref, table_sem.at[0]),
        pltpu.make_async_copy(low_any, low_ref, table_sem.at[1]),
    ]
    for copy in tables:
        copy.start()

    barrier = pltpu.get_barrier_semaphore()

    def greet(d, carry):
        pl.semaphore_signal(barrier, inc=1, device_id=(fg, (p + d) % devices), device_id_type=MESH)
        return carry

    def greet_frames(d, carry):
        there = (fg + d) % groups
        pl.semaphore_signal(barrier, inc=1, device_id=(there, p), device_id_type=MESH)
        pl.semaphore_signal(barrier, inc=1, device_id=(there, 2 * z + 1 - core), device_id_type=MESH)
        return carry

    lax.fori_loop(1, devices, greet, 0)
    lax.fori_loop(1, groups, greet_frames, 0)
    pl.semaphore_wait(barrier, devices - 1 + 2 * (groups - 1))

    def c1_copy(d):
        to = (p + d) % devices
        src = pl.ds(pl.multiple_of((to % 2) * half + fg * 8, 8), 8)
        return pltpu.make_async_remote_copy(
            src_ref=count_ref.at[src, :], dst_ref=c1.at[p], send_sem=c1_send.at[d], recv_sem=c1_recv.at[d],
            device_id=(fg, to), device_id_type=MESH,
        )

    def c1_start(d, carry):
        c1_copy(d).start()
        return carry

    lax.fori_loop(1, devices, c1_start, 0)

    def pair_copy(i):
        at = pl.ds(pl.multiple_of(i * part, 8), part)
        src = pl.ds(pl.multiple_of((1 - core) * half + i * part, 8), part)
        return pltpu.make_async_remote_copy(
            src_ref=cake_ref.at[src], dst_ref=other.at[at], send_sem=pair_send.at[i], recv_sem=pair_recv.at[i],
            device_id=(fg, 2 * z + 1 - core), device_id_type=MESH,
        )

    for i in range(PARTS):
        pair_copy(i).start()

    c1[p] = count_ref[pl.ds(pl.multiple_of(core * half + fg * 8, 8), 8), :]

    def c1_wait(d, carry):
        c1_copy(d).wait()
        return carry

    lax.fori_loop(1, devices, c1_wait, 0)
    total = c1[0]
    for i in range(1, devices):
        total = total + c1[i]
    here = pl.ds(pl.multiple_of(fg * 8, 8), 8)
    c2[here, :] = total

    def c2_copy(d):
        return pltpu.make_async_remote_copy(
            src_ref=c2.at[here, :], dst_ref=c2.at[here, :], send_sem=c2_send.at[d], recv_sem=c2_recv.at[d],
            device_id=((fg + d) % groups, p), device_id_type=MESH,
        )

    def c2_landing(d):
        at = pl.ds(pl.multiple_of((fg + groups - d) % groups * 8, 8), 8)
        return pltpu.make_async_remote_copy(
            src_ref=c2.at[here, :], dst_ref=c2.at[at, :], send_sem=c2_send.at[d], recv_sem=c2_recv.at[d],
            device_id=((fg + d) % groups, p), device_id_type=MESH,
        )

    def c2_start(d, carry):
        c2_copy(d).start()
        return carry

    def c2_wait(d, carry):
        c2_copy(d).wait_send()
        c2_landing(d).wait_recv()
        return carry

    lax.fori_loop(1, groups, c2_start, 0)
    lax.fori_loop(1, groups, c2_wait, 0)
    inverse[...] = 1.0 / jnp.maximum(c2[...], 1.0)

    for copy in tables:
        copy.wait()
    for i in range(PARTS):
        pair_copy(i).wait()

    def ring_copy(k, s):
        sign = 1 - 2 * (k % 2)
        block = (z - sign * (1 + s) + 2 * chips) % chips
        at = pl.ds(pl.multiple_of(block * rows, 8), rows)
        return pltpu.make_async_remote_copy(
            src_ref=spectra.at[k, at, :], dst_ref=arrived.at[k, s],
            send_sem=ring_send.at[k, s], recv_sem=ring_recv.at[k, s],
            device_id=(fg, 2 * ((z + sign + chips) % chips) + core), device_id_type=MESH,
        )

    def transform(g, carry):
        fs = pl.ds(pl.multiple_of(g * 8, 8), 8)

        def normalise(b, carry):
            qs = pl.ds(pl.multiple_of(b * 16, 16), 16)
            mine_qs = pl.ds(pl.multiple_of(core * half + b * 16, 16), 16)
            both = jnp.swapaxes(cake_ref[mine_qs, fs, :] + other[qs, fs, :], 0, 1) * inverse[qs, :][None]
            h, l = halves(both)
            high_in[:, qs, :] = h
            low_in[:, qs, :] = l
            return carry

        lax.fori_loop(0, half // 16, normalise, 0)
        for i in range(8 // per):
            k = g * (8 // per) + i
            for t in range(0, per, 2):
                pick = slice(i * per + t, i * per + t + 2)
                h = high_in[pick].reshape(2 * half, NCHI)
                l = low_in[pick].reshape(2 * half, NCHI)
                spectra[k, :, t * half:(t + 2) * half] = (
                    dot(high_ref[...], h, NT) + dot(high_ref[...], l, NT) + dot(low_ref[...], h, NT)
                )
            ring_copy(k, 0).start()
        return carry

    lax.fori_loop(0, frames // 8, transform, 0)

    def take(k, s):
        sign = 1 - 2 * (k % 2)
        block = (z - sign * (2 + s) + 2 * chips) % chips
        at = pl.ds(pl.multiple_of(block * rows, 8), rows)
        ring_copy(k, s).wait_recv()
        spectra[k, at, :] = spectra[k, at, :] + arrived[k, s]

    def ring_step(n, carry):
        s = n // SUBS
        k = n % SUBS
        take(k, s)
        ring_copy(k, s + 1).start()
        return carry

    lax.fori_loop(0, (chips - 2) * SUBS, ring_step, 0)

    def z_copy(g, d):
        to = (fg + d) % groups
        fs = pl.ds(pl.multiple_of(g * 8, 8), 8)
        return pltpu.make_async_remote_copy(
            src_ref=sent.at[pl.ds(2 * to, 2), fs, :], dst_ref=mine.at[fg, :, fs, :],
            send_sem=z_send.at[g, d], recv_sem=z_recv.at[g, d],
            device_id=(to, p), device_id_type=MESH,
        )

    def z_landing(g, d):
        fs = pl.ds(pl.multiple_of(g * 8, 8), 8)
        return pltpu.make_async_remote_copy(
            src_ref=sent.at[pl.ds(0, 2), fs, :], dst_ref=mine.at[(fg + groups - d) % groups, :, fs, :],
            send_sem=z_send.at[g, d], recv_sem=z_recv.at[g, d],
            device_id=((fg + d) % groups, p), device_id_type=MESH,
        )

    pack = 8 // per

    def finish(g, carry):
        for i in range(pack):
            take(g * pack + i, chips - 2)
        for t in range(rows // 8):
            at = pl.ds(pl.multiple_of(z * rows + t * 8, 8), 8)
            pieces = [
                spectra[g * pack + i, at, f * half:(f + 1) * half] for i in range(pack) for f in range(per)
            ]
            turned = jnp.swapaxes(jnp.stack(pieces, 0), 0, 1)
            sent[t * 8:t * 8 + 8, pl.ds(pl.multiple_of(g * 8, 8), 8), :] = turned

        def z_start(d, carry):
            z_copy(g, d).start()
            return carry

        lax.fori_loop(1, groups, z_start, 0)
        fs = pl.ds(pl.multiple_of(g * 8, 8), 8)
        mine[fg, :, fs, :] = sent[pl.ds(2 * fg, 2), fs, :]
        return carry

    lax.fori_loop(0, frames // 8, finish, 0)

    def swap_copy(g):
        fs = pl.ds(pl.multiple_of(g * 8, 8), 8)
        return pltpu.make_async_remote_copy(
            src_ref=mine.at[:, :, fs, :], dst_ref=theirs.at[:, :, fs, :],
            send_sem=swap_send.at[g], recv_sem=swap_recv.at[g],
            device_id=(fg, 2 * z + 1 - core), device_id_type=MESH,
        )

    scale = 1.0 / math.sqrt(groups * frames)

    def pieces_of(ref, g):
        fs = pl.ds(pl.multiple_of(g * 8, 8), 8)
        real = halves(ref[:, 0, fs, :].reshape(groups * 8, half))
        imag = halves(ref[:, 1, fs, :].reshape(groups * 8, half))
        return real, imag

    def product(g, ref):
        real, imag = pieces_of(mine, g)
        left = [
            jnp.concatenate([jnp.concatenate([r, i], 1), jnp.concatenate([i, -r], 1)], 0)
            for r, i in zip(real, imag)
        ]
        right = [jnp.concatenate([r, i], 0) for r, i in zip(*pieces_of(ref, g))]
        return (
            (dot(left[0], right[0], TN) + dot(left[0], right[1], TN) + dot(left[1], right[0], TN)) * scale
        ).reshape(2, half, half)

    corr[...] = jnp.zeros_like(corr)

    def other_half(g):
        swap_copy(g).wait_recv()
        corr[1 - core] = corr[1 - core] + product(g, theirs)

    def correlate(g, carry):
        def z_wait(d, carry):
            z_landing(g, d).wait_recv()
            return carry

        lax.fori_loop(1, groups, z_wait, 0)
        swap_copy(g).start()
        corr[core] = corr[core] + product(g, mine)

        @pl.when(g > 0)
        def _():
            other_half(g - 1)

        return carry

    lax.fori_loop(0, frames // 8, correlate, 0)
    other_half(frames // 8 - 1)

    block = NQ // groups
    blocks = groups // 2
    owner_core = fg // blocks

    def out_copy(i):
        return pltpu.make_async_remote_copy(
            src_ref=corr.at[:, :, pl.ds(pl.multiple_of(i * block, 8), block), :], dst_ref=landed.at[fg % blocks],
            send_sem=out_send.at[i], recv_sem=out_recv.at[fg % blocks],
            device_id=(core * blocks + i, 2 * z + owner_core), device_id_type=MESH,
        )

    def out_landing(n):
        return pltpu.make_async_remote_copy(
            src_ref=corr.at[:, :, pl.ds(0, block), :], dst_ref=landed.at[n],
            send_sem=out_send.at[n], recv_sem=out_recv.at[n],
            device_id=(core * blocks + n, 2 * z + owner_core), device_id_type=MESH,
        )

    def out_start(i, carry):
        @pl.when(core * blocks + i != fg)
        def _():
            out_copy(i).start()

        return carry

    lax.fori_loop(0, blocks, out_start, 0)

    @pl.when(owner_core == core)
    def _():
        i = fg % blocks
        keep = pltpu.make_async_copy(
            corr.at[:, :, pl.ds(pl.multiple_of(i * block, 8), block), :], landed.at[i], self_sem
        )
        keep.start()
        keep.wait()

    def out_wait(n, carry):
        @pl.when(core * blocks + n != fg)
        def _():
            out_landing(n).wait_recv()
            out_copy(n).wait_send()

        return carry

    lax.fori_loop(0, blocks, out_wait, 0)
    out_ref[...] = landed[...]

    for g in range(frames // 8):
        swap_copy(g).wait_send()

    def ring_done(n, carry):
        ring_copy(n % SUBS, n // SUBS).wait_send()
        return carry

    lax.fori_loop(0, (chips - 1) * SUBS, ring_done, 0)

    def z_done(n, carry):
        z_copy(n // (groups - 1), 1 + n % (groups - 1)).wait_send()
        return carry

    lax.fori_loop(0, frames // 8 * (groups - 1), z_done, 0)


def linked(cake, counts, chips, groups):
    frames = cake.shape[1]
    devices = 2 * chips
    half = NQ // 2
    part = half // PARTS
    per = frames // SUBS
    rows = 2 * NH // chips
    block = NQ // groups
    blocks = groups // 2
    high, low = fourier_table()
    f32, bf = jnp.float32, jnp.bfloat16
    dma = pltpu.SemaphoreType.DMA
    away = pl.BlockSpec(memory_space=pltpu.HBM)
    vmem = pl.BlockSpec(memory_space=pltpu.VMEM)
    return pl.pallas_call(
        lambda *refs: link_kernel(chips, groups, *refs),
        out_shape=jax.ShapeDtypeStruct((blocks, 2, 2, block, half), f32),
        in_specs=[vmem, vmem, away, away],
        out_specs=vmem,
        scratch_shapes=[
            pltpu.VMEM((2 * NH, NCHI), bf),
            pltpu.VMEM((2 * NH, NCHI), bf),
            pltpu.VMEM((half, frames, NCHI), f32),
            pltpu.VMEM((8, half, NCHI), bf),
            pltpu.VMEM((8, half, NCHI), bf),
            pltpu.VMEM((SUBS, 2 * NH, per * half), f32),
            pltpu.VMEM((SUBS, chips - 1, rows, per * half), f32),
            pltpu.VMEM((devices, 8, NCHI), f32),
            pltpu.VMEM((half, NCHI), f32),
            pltpu.VMEM((half, NCHI), f32),
            pltpu.VMEM((rows, frames, half), f32),
            pltpu.VMEM((groups, 2, frames, half), f32),
            pltpu.VMEM((groups, 2, frames, half), f32),
            pltpu.VMEM((2, 2, half, half), f32),
            pltpu.VMEM((blocks, 2, 2, block, half), f32),
            dma((2,)), dma((PARTS,)), dma((PARTS,)),
            dma((devices,)), dma((devices,)), dma((groups,)), dma((groups,)),
            dma((SUBS, chips - 1)), dma((SUBS, chips - 1)),
            dma((frames // 8, groups)), dma((frames // 8, groups)),
            dma((frames // 8,)), dma((frames // 8,)), dma((blocks,)), dma((blocks,)), dma(()),
        ],
        compiler_params=pltpu.CompilerParams(
            collective_id=0, has_side_effects=True, vmem_limit_bytes=LINK_VMEM
        ),
        name="links",
    )(cake, counts, stay(jnp.asarray(high)), stay(jnp.asarray(low)))


def fourier_table():
    harmonic = np.arange(NH)[:, None]
    phases = (harmonic * np.arange(NCHI)[None, :] % NCHI) * (2.0 * math.pi / NCHI)
    table = np.stack([np.cos(phases), -np.sin(phases)], 1) / math.sqrt(NCHI)
    table = table.reshape(2 * NH, NCHI).astype(np.float32)
    high = table.astype(jnp.bfloat16)
    return high, (table - high.astype(np.float32)).astype(jnp.bfloat16)


def solution(mesh):
    groups = mesh.shape["frames"]
    chips = mesh.shape["pix"] // 2

    def body(intensity, chi_bin, split, mask, tile_row):
        cake, counts = binned(intensity, chi_bin, split, mask, tile_row)
        blocks = linked(cake, counts, chips, groups)
        n, h, c, q, r = blocks.shape
        return blocks.transpose(3, 2, 0, 1, 4).reshape(q, c, n, h * r)

    in_specs = (P("frames", "pix"), P("pix"), P("pix"), P("pix"), P("pix"))
    out_specs = P("frames", None, "pix", None)
    return jax.shard_map(body, mesh=mesh, in_specs=in_specs, out_specs=out_specs, check_vma=False)
```

```python
import math

import jax
import jax.numpy as jnp
import numpy as np
from jax import lax
from jax.experimental import pallas as pl
from jax.experimental.pallas import tpu as pltpu
from jax.sharding import PartitionSpec as P

NQ = 256
NCHI = 256
NH = 128
ROWS = 40
TILE_BLOCK = 64
GROUP = 32
BIN_VMEM = 36 << 20
LINK_VMEM = 36 << 20
MESH = pl.DeviceIdType.MESH
SUBS = 8
UNROLL = 5
PARTS = 4
TN = (((0,), (0,)), ((), ()))
NT = (((1,), (1,)), ((), ()))


def bin_kernel(
    rows_any, x_any, chi_any, split_any, mask_any, cake_ref, count_ref,
    rows_ref, x_ref, chi_ref, split_ref, mask_ref, count_acc, vals, rows_sem, sem,
):
    frames = x_ref.shape[0]
    tiles = chi_ref.shape[0]
    blocks = tiles // TILE_BLOCK
    bf = jnp.bfloat16

    def copies(b):
        at = pl.ds(pl.multiple_of(b * TILE_BLOCK, 8), TILE_BLOCK)
        wide = pl.ds(pl.multiple_of(b * TILE_BLOCK * 128, 128), TILE_BLOCK * 128)
        pairs = ((chi_any, chi_ref), (split_any, split_ref), (mask_any, mask_ref))
        flat = [pltpu.make_async_copy(a.at[at, :], r.at[at, :], sem.at[b, n]) for n, (a, r) in enumerate(pairs)]
        return flat + [pltpu.make_async_copy(x_any.at[:, wide], x_ref.at[:, wide], sem.at[b, 3])]

    rows_copy = pltpu.make_async_copy(rows_any, rows_ref, rows_sem)
    rows_copy.start()
    for b in range(blocks):
        for copy in copies(b):
            copy.start()

    def clear(n, carry):
        at = pl.ds(n * 8, 8)
        cake_ref[at] = jnp.zeros((8, frames, NCHI), jnp.float32)
        count_acc[at] = jnp.zeros((8, 8, NCHI), jnp.float32)
        return carry

    lax.fori_loop(0, NQ // 8, clear, 0)
    vals[...] = jnp.zeros_like(vals)

    zero = jnp.zeros((), bf)
    columns = lax.broadcasted_iota(jnp.int32, (NCHI, 128), 0).astype(jnp.float32).astype(bf)
    row = lax.broadcasted_iota(jnp.int32, (16, 256), 0)
    lane = lax.broadcasted_iota(jnp.int32, (16, 256), 1)
    ones = jnp.where(((row == 0) & (lane < 128)) | ((row == 8) & (lane >= 128)), 1.0, 0.0).astype(bf)
    blank = jnp.zeros((frames, 128), bf)

    def weights_of(t):
        chi = chi_ref[pl.ds(t, 1), :]
        usable = mask_ref[pl.ds(t, 1), :].astype(jnp.float32)
        split = split_ref[pl.ds(t, 1), :]
        near = (usable * split).astype(bf)
        far = (usable * (1.0 - split)).astype(bf)
        here = chi.astype(jnp.float32).astype(bf)
        after = ((chi + 1) & (NCHI - 1)).astype(jnp.float32).astype(bf)
        return jnp.where(columns == here, near, jnp.where(columns == after, far, zero))

    def add(first, slot):
        for u in range(GROUP):
            q = rows_ref[first + u]
            cake_ref[q] = cake_ref[q] + vals[slot, u, :frames]
            count_acc[q] = count_acc[q] + vals[slot, u, frames:]

    def group(g, carry):
        slot = lax.rem(g, 2)

        @pl.when(lax.rem(g * GROUP, TILE_BLOCK) == 0)
        def _():
            for copy in copies(g * GROUP // TILE_BLOCK):
                copy.wait()

        for u in range(0, GROUP, 2):
            t = g * GROUP + u
            weights = jnp.concatenate([weights_of(t), weights_of(t + 1)], axis=1)
            a = x_ref[:, pl.ds(pl.multiple_of(t * 128, 128), 128)]
            b = x_ref[:, pl.ds(pl.multiple_of(t * 128 + 128, 128), 128)]
            left = jnp.concatenate(
                [jnp.concatenate([a, blank], 1), jnp.concatenate([blank, b], 1), ones], axis=0
            )
            value = dot(left, weights, NT)
            vals[slot, u, :frames] = value[:frames]
            vals[slot, u, frames:] = value[2 * frames:2 * frames + 8]
            vals[slot, u + 1, :frames] = value[frames:2 * frames]
            vals[slot, u + 1, frames:] = value[2 * frames + 8:]
        add(jnp.maximum((g - 1) * GROUP, 0), 1 - slot)
        return carry

    rows_copy.wait()
    groups = tiles // GROUP
    lax.fori_loop(0, groups, group, 0)
    add(tiles - GROUP, (groups - 1) % 2)

    def rows_of(b, carry):
        at = pl.ds(pl.multiple_of(b * 8, 8), 8)
        count_ref[at, :] = count_acc[at, 0, :]
        return carry

    lax.fori_loop(0, NQ // 8, rows_of, 0)


def stay(a):
    return pltpu.with_memory_space_constraint(a, pltpu.HBM)


def binned(intensity, chi_bin, split, mask, tile_row):
    frames, pixels = intensity.shape
    tiles = tile_row.shape[0]
    vmem = pl.BlockSpec(memory_space=pltpu.VMEM)
    away = pl.BlockSpec(memory_space=pltpu.HBM)
    return pl.pallas_call(
        bin_kernel,
        out_shape=(
            jax.ShapeDtypeStruct((NQ, frames, NCHI), jnp.float32),
            jax.ShapeDtypeStruct((NQ, NCHI), jnp.float32),
        ),
        in_specs=[away, away, away, away, away],
        out_specs=(vmem, vmem),
        scratch_shapes=[
            pltpu.SMEM((tiles,), jnp.int32),
            pltpu.VMEM((frames, pixels), jnp.bfloat16),
            pltpu.VMEM((tiles, 128), jnp.int32),
            pltpu.VMEM((tiles, 128), jnp.float32),
            pltpu.VMEM((tiles, 128), jnp.int32),
            pltpu.VMEM((NQ, 8, NCHI), jnp.float32),
            pltpu.VMEM((2, GROUP, ROWS, NCHI), jnp.float32),
            pltpu.SemaphoreType.DMA,
            pltpu.SemaphoreType.DMA((tiles // TILE_BLOCK, 4)),
        ],
        compiler_params=pltpu.CompilerParams(vmem_limit_bytes=BIN_VMEM),
        name="binning",
    )(*(stay(a) for a in (tile_row, intensity, *(a.reshape(tiles, 128) for a in (chi_bin, split, mask)))))


def halves(x):
    high = x.astype(jnp.bfloat16)
    return high, (x - high.astype(jnp.float32)).astype(jnp.bfloat16)


def dot(a, b, dims):
    return lax.dot_general(a, b, dims, preferred_element_type=jnp.float32)


def link_kernel(
    chips, groups, cake_ref, count_ref, high_any, low_any, out_ref,
    high_ref, low_ref, other, raw, spectra, arrived, c1, c2, inverse,
    sent, mine, theirs, corr, landed,
    table_sem, pair_send, pair_recv, c1_send, c1_recv, c2_send, c2_recv,
    ring_send, ring_recv, z_send, z_recv, swap_send, swap_recv, out_send, out_recv, self_sem,
):
    fg = lax.axis_index("frames")
    p = lax.axis_index("pix")
    z = p // 2
    core = p % 2
    devices = 2 * chips
    frames = cake_ref.shape[1]
    half = NQ // 2
    part = half // PARTS
    per = frames // SUBS
    rows = 2 * NH // chips
    lanes = per * half

    tables = [
        pltpu.make_async_copy(high_any, high_ref, table_sem.at[0]),
        pltpu.make_async_copy(low_any, low_ref, table_sem.at[1]),
    ]
    for copy in tables:
        copy.start()

    barrier = pltpu.get_barrier_semaphore()

    def greet(d, carry):
        pl.semaphore_signal(barrier, inc=1, device_id=(fg, (p + d) % devices), device_id_type=MESH)
        return carry

    def greet_frames(d, carry):
        pl.semaphore_signal(barrier, inc=1, device_id=((fg + d) % groups, p), device_id_type=MESH)
        return carry

    def greet_owners(i, carry):
        to = core * (groups // 2) + i
        pl.semaphore_signal(barrier, inc=1, device_id=(to, 2 * z + 1 - core), device_id_type=MESH)
        return carry

    lax.fori_loop(1, devices, greet, 0, unroll=UNROLL)
    lax.fori_loop(1, groups, greet_frames, 0, unroll=UNROLL)

    @pl.when(fg // (groups // 2) != core)
    def _():
        lax.fori_loop(0, groups // 2, greet_owners, 0, unroll=UNROLL)

    apart = fg // (groups // 2) - core
    pl.semaphore_wait(barrier, devices + groups - 2 + groups // 2 * apart * apart)

    def c1_copy(d):
        to = (p + d) % devices
        src = pl.ds(pl.multiple_of((to % 2) * half + fg * 8, 8), 8)
        return pltpu.make_async_remote_copy(
            src_ref=count_ref.at[src, :], dst_ref=c1.at[p], send_sem=c1_send.at[d], recv_sem=c1_recv.at[d],
            device_id=(fg, to), device_id_type=MESH,
        )

    def c1_start(d, carry):
        c1_copy(d).start()
        return carry

    lax.fori_loop(1, devices, c1_start, 0, unroll=UNROLL)

    def pair_copy(i):
        at = pl.ds(pl.multiple_of(i * part, 8), part)
        src = pl.ds(pl.multiple_of((1 - core) * half + i * part, 8), part)
        return pltpu.make_async_remote_copy(
            src_ref=cake_ref.at[src], dst_ref=other.at[at], send_sem=pair_send.at[i], recv_sem=pair_recv.at[i],
            device_id=(fg, 2 * z + 1 - core), device_id_type=MESH,
        )

    for i in range(PARTS):
        pair_copy(i).start()

    c1[p] = count_ref[pl.ds(pl.multiple_of(core * half + fg * 8, 8), 8), :]

    def c1_wait(d, carry):
        c1_copy(d).wait()
        return carry

    lax.fori_loop(1, devices, c1_wait, 0, unroll=UNROLL)
    total = c1[0]
    for i in range(1, devices):
        total = total + c1[i]
    here = pl.ds(pl.multiple_of(fg * 8, 8), 8)
    c2[here, :] = total

    def c2_copy(d):
        return pltpu.make_async_remote_copy(
            src_ref=c2.at[here, :], dst_ref=c2.at[here, :], send_sem=c2_send.at[d], recv_sem=c2_recv.at[d],
            device_id=((fg + d) % groups, p), device_id_type=MESH,
        )

    def c2_landing(d):
        at = pl.ds(pl.multiple_of((fg + groups - d) % groups * 8, 8), 8)
        return pltpu.make_async_remote_copy(
            src_ref=c2.at[here, :], dst_ref=c2.at[at, :], send_sem=c2_send.at[d], recv_sem=c2_recv.at[d],
            device_id=((fg + d) % groups, p), device_id_type=MESH,
        )

    def c2_start(d, carry):
        c2_copy(d).start()
        return carry

    def c2_wait(d, carry):
        c2_copy(d).wait_send()
        c2_landing(d).wait_recv()
        return carry

    lax.fori_loop(1, groups, c2_start, 0, unroll=UNROLL)

    for copy in tables:
        copy.wait()
    for i in range(PARTS):
        pair_copy(i).wait()

    def gather(n, carry):
        b = n // (frames // 8)
        qs = pl.ds(pl.multiple_of(b * 16, 16), 16)
        mine_qs = pl.ds(pl.multiple_of(core * half + b * 16, 16), 16)
        fs = pl.ds(pl.multiple_of(n % (frames // 8) * 8, 8), 8)
        raw[fs, qs, :] = jnp.swapaxes(cake_ref[mine_qs, fs, :] + other[qs, fs, :], 0, 1)
        return carry

    lax.fori_loop(0, half // 16 * (frames // 8), gather, 0)
    lax.fori_loop(1, groups, c2_wait, 0, unroll=UNROLL)
    inverse[...] = 1.0 / jnp.maximum(c2[...], 1.0)

    def ring_copy(k, s):
        sign = 1 - 2 * (k % 2)
        block = (z - sign * (1 + s) + 2 * chips) % chips
        at = pl.ds(pl.multiple_of(block * rows, 8), rows)
        return pltpu.make_async_remote_copy(
            src_ref=spectra.at[k, at, :], dst_ref=arrived.at[k, s],
            send_sem=ring_send.at[k, s], recv_sem=ring_recv.at[k, s],
            device_id=(fg, 2 * ((z + sign + chips) % chips) + core), device_id_type=MESH,
        )

    def transform(k, carry):
        for t in range(0, per, 2):
            cakes = raw[pl.ds(k * per + t, 2)] * inverse[...][None]
            h, l = halves(cakes.reshape(2 * half, NCHI))
            spectra[k, :, t * half:(t + 2) * half] = (
                dot(high_ref[...], h, NT) + dot(high_ref[...], l, NT) + dot(low_ref[...], h, NT)
            )
        ring_copy(k, 0).start()
        return carry

    lax.fori_loop(0, SUBS, transform, 0)

    def take(k, s):
        sign = 1 - 2 * (k % 2)
        block = (z - sign * (2 + s) + 2 * chips) % chips
        at = pl.ds(pl.multiple_of(block * rows, 8), rows)
        ring_copy(k, s).wait_recv()
        spectra[k, at, :] = spectra[k, at, :] + arrived[k, s]

    def ring_step(n, carry):
        s = n // SUBS
        k = n % SUBS
        take(k, s)
        ring_copy(k, s + 1).start()
        return carry

    lax.fori_loop(0, (chips - 2) * SUBS, ring_step, 0)

    def z_copy(g, d):
        to = (fg + d) % groups
        fs = pl.ds(pl.multiple_of(g * 8, 8), 8)
        return pltpu.make_async_remote_copy(
            src_ref=sent.at[pl.ds(2 * to, 2), fs, :], dst_ref=mine.at[fg, :, fs, :],
            send_sem=z_send.at[g, d], recv_sem=z_recv.at[g, d],
            device_id=(to, p), device_id_type=MESH,
        )

    def z_landing(g, d):
        fs = pl.ds(pl.multiple_of(g * 8, 8), 8)
        return pltpu.make_async_remote_copy(
            src_ref=sent.at[pl.ds(0, 2), fs, :], dst_ref=mine.at[(fg + groups - d) % groups, :, fs, :],
            send_sem=z_send.at[g, d], recv_sem=z_recv.at[g, d],
            device_id=((fg + d) % groups, p), device_id_type=MESH,
        )

    pack = 8 // per

    def finish(g, carry):
        for i in range(pack):
            take(g * pack + i, chips - 2)
        for t in range(rows // 8):
            at = pl.ds(pl.multiple_of(z * rows + t * 8, 8), 8)
            pieces = [
                spectra[g * pack + i, at, f * half:(f + 1) * half] for i in range(pack) for f in range(per)
            ]
            turned = jnp.swapaxes(jnp.stack(pieces, 0), 0, 1)
            sent[t * 8:t * 8 + 8, pl.ds(pl.multiple_of(g * 8, 8), 8), :] = turned

        def z_start(d, carry):
            z_copy(g, d).start()
            return carry

        lax.fori_loop(1, groups, z_start, 0, unroll=UNROLL)
        fs = pl.ds(pl.multiple_of(g * 8, 8), 8)
        mine[fg, :, fs, :] = sent[pl.ds(2 * fg, 2), fs, :]
        return carry

    lax.fori_loop(0, frames // 8, finish, 0)

    def swap_copy(g):
        fs = pl.ds(pl.multiple_of(g * 8, 8), 8)
        return pltpu.make_async_remote_copy(
            src_ref=mine.at[:, :, fs, :], dst_ref=theirs.at[:, :, fs, :],
            send_sem=swap_send.at[g], recv_sem=swap_recv.at[g],
            device_id=(fg, 2 * z + 1 - core), device_id_type=MESH,
        )

    scale = 1.0 / math.sqrt(groups * frames)

    def pieces_of(ref, g):
        fs = pl.ds(pl.multiple_of(g * 8, 8), 8)
        real = halves(ref[:, 0, fs, :].reshape(groups * 8, half))
        imag = halves(ref[:, 1, fs, :].reshape(groups * 8, half))
        return real, imag

    def product(g, ref):
        real, imag = pieces_of(mine, g)
        left = [
            jnp.concatenate([jnp.concatenate([r, i], 1), jnp.concatenate([i, -r], 1)], 0)
            for r, i in zip(real, imag)
        ]
        right = [jnp.concatenate([r, i], 0) for r, i in zip(*pieces_of(ref, g))]
        return (
            (dot(left[0], right[0], TN) + dot(left[0], right[1], TN) + dot(left[1], right[0], TN)) * scale
        ).reshape(2, half, half)

    corr[...] = jnp.zeros_like(corr)

    def other_half(g):
        swap_copy(g).wait_recv()
        corr[1 - core] = corr[1 - core] + product(g, theirs)

    def ring_done(n, carry):
        ring_copy(n % SUBS, n // SUBS).wait_send()
        return carry

    lax.fori_loop(0, (chips - 1) * SUBS, ring_done, 0)

    def correlate(g, carry):
        def z_wait(d, carry):
            z_landing(g, d).wait_recv()
            return carry

        lax.fori_loop(1, groups, z_wait, 0, unroll=UNROLL)
        swap_copy(g).start()
        corr[core] = corr[core] + product(g, mine)

        @pl.when(g > 0)
        def _():
            other_half(g - 1)

        return carry

    lax.fori_loop(0, frames // 8, correlate, 0)
    other_half(frames // 8 - 1)

    block = NQ // groups
    blocks = groups // 2
    owner_core = fg // blocks

    def out_copy(i):
        return pltpu.make_async_remote_copy(
            src_ref=corr.at[:, :, pl.ds(pl.multiple_of(i * block, 8), block), :], dst_ref=landed.at[fg % blocks],
            send_sem=out_send.at[i], recv_sem=out_recv.at[fg % blocks],
            device_id=(core * blocks + i, 2 * z + owner_core), device_id_type=MESH,
        )

    def out_landing(n):
        return pltpu.make_async_remote_copy(
            src_ref=corr.at[:, :, pl.ds(0, block), :], dst_ref=landed.at[n],
            send_sem=out_send.at[n], recv_sem=out_recv.at[n],
            device_id=(core * blocks + n, 2 * z + owner_core), device_id_type=MESH,
        )

    def out_start(i, carry):
        @pl.when(core * blocks + i != fg)
        def _():
            out_copy(i).start()

        return carry

    lax.fori_loop(0, blocks, out_start, 0)

    for g in range(frames // 8):
        swap_copy(g).wait_send()

    def z_done(n, carry):
        z_copy(n // (groups - 1), 1 + n % (groups - 1)).wait_send()
        return carry

    lax.fori_loop(0, frames // 8 * (groups - 1), z_done, 0)

    @pl.when(owner_core == core)
    def _():
        i = fg % blocks
        keep = pltpu.make_async_copy(
            corr.at[:, :, pl.ds(pl.multiple_of(i * block, 8), block), :], landed.at[i], self_sem
        )
        keep.start()
        keep.wait()

    def out_wait(n, carry):
        @pl.when(core * blocks + n != fg)
        def _():
            out_landing(n).wait_recv()
            out_copy(n).wait_send()

        return carry

    lax.fori_loop(0, blocks, out_wait, 0)
    out_ref[...] = landed[...]


def linked(cake, counts, chips, groups):
    frames = cake.shape[1]
    devices = 2 * chips
    half = NQ // 2
    part = half // PARTS
    per = frames // SUBS
    rows = 2 * NH // chips
    block = NQ // groups
    blocks = groups // 2
    high, low = fourier_table()
    f32, bf = jnp.float32, jnp.bfloat16
    dma = pltpu.SemaphoreType.DMA
    away = pl.BlockSpec(memory_space=pltpu.HBM)
    vmem = pl.BlockSpec(memory_space=pltpu.VMEM)
    return pl.pallas_call(
        lambda *refs: link_kernel(chips, groups, *refs),
        out_shape=jax.ShapeDtypeStruct((blocks, 2, 2, block, half), f32),
        in_specs=[vmem, vmem, away, away],
        out_specs=vmem,
        scratch_shapes=[
            pltpu.VMEM((2 * NH, NCHI), bf),
            pltpu.VMEM((2 * NH, NCHI), bf),
            pltpu.VMEM((half, frames, NCHI), f32),
            pltpu.VMEM((frames, half, NCHI), f32),
            pltpu.VMEM((SUBS, 2 * NH, per * half), f32),
            pltpu.VMEM((SUBS, chips - 1, rows, per * half), f32),
            pltpu.VMEM((devices, 8, NCHI), f32),
            pltpu.VMEM((half, NCHI), f32),
            pltpu.VMEM((half, NCHI), f32),
            pltpu.VMEM((rows, frames, half), f32),
            pltpu.VMEM((groups, 2, frames, half), f32),
            pltpu.VMEM((groups, 2, frames, half), f32),
            pltpu.VMEM((2, 2, half, half), f32),
            pltpu.VMEM((blocks, 2, 2, block, half), f32),
            dma((2,)), dma((PARTS,)), dma((PARTS,)),
            dma((devices,)), dma((devices,)), dma((groups,)), dma((groups,)),
            dma((SUBS, chips - 1)), dma((SUBS, chips - 1)),
            dma((frames // 8, groups)), dma((frames // 8, groups)),
            dma((frames // 8,)), dma((frames // 8,)), dma((blocks,)), dma((blocks,)), dma(()),
        ],
        compiler_params=pltpu.CompilerParams(
            collective_id=0, has_side_effects=True, vmem_limit_bytes=LINK_VMEM
        ),
        name="links",
    )(cake, counts, stay(jnp.asarray(high)), stay(jnp.asarray(low)))


def fourier_table():
    harmonic = np.arange(NH)[:, None]
    phases = (harmonic * np.arange(NCHI)[None, :] % NCHI) * (2.0 * math.pi / NCHI)
    table = np.stack([np.cos(phases), -np.sin(phases)], 1) / math.sqrt(NCHI)
    table = table.reshape(2 * NH, NCHI).astype(np.float32)
    high = table.astype(jnp.bfloat16)
    return high, (table - high.astype(np.float32)).astype(jnp.bfloat16)


def solution(mesh):
    groups = mesh.shape["frames"]
    chips = mesh.shape["pix"] // 2

    def body(intensity, chi_bin, split, mask, tile_row):
        cake, counts = binned(intensity, chi_bin, split, mask, tile_row)
        blocks = linked(cake, counts, chips, groups)
        n, h, c, q, r = blocks.shape
        return blocks.transpose(3, 2, 0, 1, 4).reshape(q, c, n, h * r)

    in_specs = (P("frames", "pix"), P("pix"), P("pix"), P("pix"), P("pix"))
    out_specs = P("frames", None, "pix", None)
    return jax.shard_map(body, mesh=mesh, in_specs=in_specs, out_specs=out_specs, check_vma=False)
```

```python
import math

import jax
import jax.numpy as jnp
import numpy as np
from jax import lax
from jax.experimental import pallas as pl
from jax.experimental.pallas import tpu as pltpu
from jax.sharding import PartitionSpec as P

NQ = 256
NCHI = 256
NH = 128
ROWS = 40
TILE_BLOCK = 64
GROUP = 32
BIN_VMEM = 36 << 20
LINK_VMEM = 36 << 20
MESH = pl.DeviceIdType.MESH
SUBS = 8
UNROLL = 5
PARTS = 4
TN = (((0,), (0,)), ((), ()))
NT = (((1,), (1,)), ((), ()))


def bin_kernel(
    rows_any, x_any, chi_any, split_any, mask_any, cake_ref, count_ref,
    rows_ref, x_ref, chi_ref, split_ref, mask_ref, count_acc, vals, rows_sem, sem,
):
    frames = x_ref.shape[0]
    tiles = chi_ref.shape[0]
    blocks = tiles // TILE_BLOCK
    bf = jnp.bfloat16

    def copies(b):
        at = pl.ds(pl.multiple_of(b * TILE_BLOCK, 8), TILE_BLOCK)
        wide = pl.ds(pl.multiple_of(b * TILE_BLOCK * 128, 128), TILE_BLOCK * 128)
        pairs = ((chi_any, chi_ref), (split_any, split_ref), (mask_any, mask_ref))
        flat = [pltpu.make_async_copy(a.at[at, :], r.at[at, :], sem.at[b, n]) for n, (a, r) in enumerate(pairs)]
        return flat + [pltpu.make_async_copy(x_any.at[:, wide], x_ref.at[:, wide], sem.at[b, 3])]

    rows_copy = pltpu.make_async_copy(rows_any, rows_ref, rows_sem)
    rows_copy.start()
    for b in range(blocks):
        for copy in copies(b):
            copy.start()

    def clear(n, carry):
        at = pl.ds(n * 8, 8)
        cake_ref[at] = jnp.zeros((8, frames, NCHI), jnp.float32)
        count_acc[at] = jnp.zeros((8, 8, NCHI), jnp.float32)
        return carry

    lax.fori_loop(0, NQ // 8, clear, 0)
    vals[...] = jnp.zeros_like(vals)

    zero = jnp.zeros((), bf)
    columns = lax.broadcasted_iota(jnp.int32, (NCHI, 128), 0).astype(jnp.float32).astype(bf)
    row = lax.broadcasted_iota(jnp.int32, (16, 256), 0)
    lane = lax.broadcasted_iota(jnp.int32, (16, 256), 1)
    ones = jnp.where(((row == 0) & (lane < 128)) | ((row == 8) & (lane >= 128)), 1.0, 0.0).astype(bf)
    blank = jnp.zeros((frames, 128), bf)

    def weights_of(t):
        chi = chi_ref[pl.ds(t, 1), :]
        usable = mask_ref[pl.ds(t, 1), :].astype(jnp.float32)
        split = split_ref[pl.ds(t, 1), :]
        near = (usable * split).astype(bf)
        far = (usable * (1.0 - split)).astype(bf)
        here = chi.astype(jnp.float32).astype(bf)
        after = ((chi + 1) & (NCHI - 1)).astype(jnp.float32).astype(bf)
        return jnp.where(columns == here, near, jnp.where(columns == after, far, zero))

    def add(first, slot):
        for u in range(GROUP):
            q = rows_ref[first + u]
            cake_ref[q] = cake_ref[q] + vals[slot, u, :frames]
            count_acc[q] = count_acc[q] + vals[slot, u, frames:]

    def group(g, carry):
        slot = lax.rem(g, 2)

        @pl.when(lax.rem(g * GROUP, TILE_BLOCK) == 0)
        def _():
            for copy in copies(g * GROUP // TILE_BLOCK):
                copy.wait()

        for u in range(0, GROUP, 2):
            t = g * GROUP + u
            weights = jnp.concatenate([weights_of(t), weights_of(t + 1)], axis=1)
            a = x_ref[:, pl.ds(pl.multiple_of(t * 128, 128), 128)]
            b = x_ref[:, pl.ds(pl.multiple_of(t * 128 + 128, 128), 128)]
            left = jnp.concatenate(
                [jnp.concatenate([a, blank], 1), jnp.concatenate([blank, b], 1), ones], axis=0
            )
            value = dot(left, weights, NT)
            vals[slot, u, :frames] = value[:frames]
            vals[slot, u, frames:] = value[2 * frames:2 * frames + 8]
            vals[slot, u + 1, :frames] = value[frames:2 * frames]
            vals[slot, u + 1, frames:] = value[2 * frames + 8:]
        add(jnp.maximum((g - 1) * GROUP, 0), 1 - slot)
        return carry

    rows_copy.wait()
    groups = tiles // GROUP
    lax.fori_loop(0, groups, group, 0)
    add(tiles - GROUP, (groups - 1) % 2)

    def rows_of(b, carry):
        at = pl.ds(pl.multiple_of(b * 8, 8), 8)
        count_ref[at, :] = count_acc[at, 0, :]
        return carry

    lax.fori_loop(0, NQ // 8, rows_of, 0)


def stay(a):
    return pltpu.with_memory_space_constraint(a, pltpu.HBM)


def binned(intensity, chi_bin, split, mask, tile_row):
    frames, pixels = intensity.shape
    tiles = tile_row.shape[0]
    vmem = pl.BlockSpec(memory_space=pltpu.VMEM)
    away = pl.BlockSpec(memory_space=pltpu.HBM)
    return pl.pallas_call(
        bin_kernel,
        out_shape=(
            jax.ShapeDtypeStruct((NQ, frames, NCHI), jnp.float32),
            jax.ShapeDtypeStruct((NQ, NCHI), jnp.float32),
        ),
        in_specs=[away, away, away, away, away],
        out_specs=(vmem, vmem),
        scratch_shapes=[
            pltpu.SMEM((tiles,), jnp.int32),
            pltpu.VMEM((frames, pixels), jnp.bfloat16),
            pltpu.VMEM((tiles, 128), jnp.int32),
            pltpu.VMEM((tiles, 128), jnp.float32),
            pltpu.VMEM((tiles, 128), jnp.int32),
            pltpu.VMEM((NQ, 8, NCHI), jnp.float32),
            pltpu.VMEM((2, GROUP, ROWS, NCHI), jnp.float32),
            pltpu.SemaphoreType.DMA,
            pltpu.SemaphoreType.DMA((tiles // TILE_BLOCK, 4)),
        ],
        compiler_params=pltpu.CompilerParams(vmem_limit_bytes=BIN_VMEM),
        name="binning",
    )(*(stay(a) for a in (tile_row, intensity, *(a.reshape(tiles, 128) for a in (chi_bin, split, mask)))))


def halves(x):
    high = x.astype(jnp.bfloat16)
    return high, (x - high.astype(jnp.float32)).astype(jnp.bfloat16)


def dot(a, b, dims):
    return lax.dot_general(a, b, dims, preferred_element_type=jnp.float32)


def far_first(d, n):
    return 1 + (d - 1 + n // 2 - 1) % (n - 1)


def link_kernel(
    chips, groups, cake_ref, count_ref, high_any, low_any, out_ref,
    high_ref, low_ref, other, raw, spectra, arrived, c1, c2, inverse,
    sent, mine, theirs, corr, landed,
    table_sem, pair_send, pair_recv, c1_send, c1_recv, c2_send, c2_recv,
    ring_send, ring_recv, z_send, z_recv, swap_send, swap_recv, out_send, out_recv, self_sem,
):
    fg = lax.axis_index("frames")
    p = lax.axis_index("pix")
    z = p // 2
    core = p % 2
    devices = 2 * chips
    frames = cake_ref.shape[1]
    half = NQ // 2
    part = half // PARTS
    per = frames // SUBS
    rows = 2 * NH // chips
    lanes = per * half

    tables = [
        pltpu.make_async_copy(high_any, high_ref, table_sem.at[0]),
        pltpu.make_async_copy(low_any, low_ref, table_sem.at[1]),
    ]
    for copy in tables:
        copy.start()

    barrier = pltpu.get_barrier_semaphore()

    def greet(d, carry):
        pl.semaphore_signal(barrier, inc=1, device_id=(fg, (p + far_first(d, devices)) % devices), device_id_type=MESH)
        return carry

    def greet_frames(d, carry):
        to = (fg + far_first(d, groups)) % groups
        pl.semaphore_signal(barrier, inc=1, device_id=(to, p), device_id_type=MESH)
        return carry

    def greet_owners(i, carry):
        to = core * (groups // 2) + i
        pl.semaphore_signal(barrier, inc=1, device_id=(to, 2 * z + 1 - core), device_id_type=MESH)
        return carry

    lax.fori_loop(1, devices, greet, 0, unroll=UNROLL)
    lax.fori_loop(1, groups, greet_frames, 0, unroll=UNROLL)

    @pl.when(fg // (groups // 2) != core)
    def _():
        lax.fori_loop(0, groups // 2, greet_owners, 0, unroll=UNROLL)

    apart = fg // (groups // 2) - core
    pl.semaphore_wait(barrier, devices + groups - 2 + groups // 2 * apart * apart)

    def c1_copy(d):
        to = (p + d) % devices
        src = pl.ds(pl.multiple_of((to % 2) * half + fg * 8, 8), 8)
        return pltpu.make_async_remote_copy(
            src_ref=count_ref.at[src, :], dst_ref=c1.at[p], send_sem=c1_send.at[d], recv_sem=c1_recv.at[d],
            device_id=(fg, to), device_id_type=MESH,
        )

    def c1_start(d, carry):
        c1_copy(far_first(d, devices)).start()
        return carry

    lax.fori_loop(1, devices, c1_start, 0, unroll=UNROLL)

    def pair_copy(i):
        at = pl.ds(pl.multiple_of(i * part, 8), part)
        src = pl.ds(pl.multiple_of((1 - core) * half + i * part, 8), part)
        return pltpu.make_async_remote_copy(
            src_ref=cake_ref.at[src], dst_ref=other.at[at], send_sem=pair_send.at[i], recv_sem=pair_recv.at[i],
            device_id=(fg, 2 * z + 1 - core), device_id_type=MESH,
        )

    for i in range(PARTS):
        pair_copy(i).start()

    c1[p] = count_ref[pl.ds(pl.multiple_of(core * half + fg * 8, 8), 8), :]

    def c1_wait(d, carry):
        c1_copy(d).wait()
        return carry

    lax.fori_loop(1, devices, c1_wait, 0, unroll=UNROLL)
    total = c1[0]
    for i in range(1, devices):
        total = total + c1[i]
    here = pl.ds(pl.multiple_of(fg * 8, 8), 8)
    c2[here, :] = total

    def c2_copy(d):
        return pltpu.make_async_remote_copy(
            src_ref=c2.at[here, :], dst_ref=c2.at[here, :], send_sem=c2_send.at[d], recv_sem=c2_recv.at[d],
            device_id=((fg + d) % groups, p), device_id_type=MESH,
        )

    def c2_landing(d):
        at = pl.ds(pl.multiple_of((fg + groups - d) % groups * 8, 8), 8)
        return pltpu.make_async_remote_copy(
            src_ref=c2.at[here, :], dst_ref=c2.at[at, :], send_sem=c2_send.at[d], recv_sem=c2_recv.at[d],
            device_id=((fg + d) % groups, p), device_id_type=MESH,
        )

    def c2_start(d, carry):
        c2_copy(far_first(d, groups)).start()
        return carry

    def c2_wait(d, carry):
        c2_copy(d).wait_send()
        c2_landing(d).wait_recv()
        return carry

    lax.fori_loop(1, groups, c2_start, 0, unroll=UNROLL)

    for copy in tables:
        copy.wait()
    for i in range(PARTS):
        pair_copy(i).wait()

    def gather(n, carry):
        b = n // (frames // 8)
        qs = pl.ds(pl.multiple_of(b * 16, 16), 16)
        mine_qs = pl.ds(pl.multiple_of(core * half + b * 16, 16), 16)
        fs = pl.ds(pl.multiple_of(n % (frames // 8) * 8, 8), 8)
        raw[fs, qs, :] = jnp.swapaxes(cake_ref[mine_qs, fs, :] + other[qs, fs, :], 0, 1)
        return carry

    lax.fori_loop(0, half // 16 * (frames // 8), gather, 0)
    lax.fori_loop(1, groups, c2_wait, 0, unroll=UNROLL)
    inverse[...] = 1.0 / jnp.maximum(c2[...], 1.0)

    def ring_copy(k, s):
        sign = 1 - 2 * (k % 2)
        block = (z - sign * (1 + s) + 2 * chips) % chips
        at = pl.ds(pl.multiple_of(block * rows, 8), rows)
        return pltpu.make_async_remote_copy(
            src_ref=spectra.at[k, at, :], dst_ref=arrived.at[k, s],
            send_sem=ring_send.at[k, s], recv_sem=ring_recv.at[k, s],
            device_id=(fg, 2 * ((z + sign + chips) % chips) + core), device_id_type=MESH,
        )

    def transform(k, carry):
        for t in range(0, per, 2):
            cakes = raw[pl.ds(k * per + t, 2)] * inverse[...][None]
            h, l = halves(cakes.reshape(2 * half, NCHI))
            spectra[k, :, t * half:(t + 2) * half] = (
                dot(high_ref[...], h, NT) + dot(high_ref[...], l, NT) + dot(low_ref[...], h, NT)
            )
        ring_copy(k, 0).start()
        return carry

    lax.fori_loop(0, SUBS, transform, 0)

    def take(k, s):
        sign = 1 - 2 * (k % 2)
        block = (z - sign * (2 + s) + 2 * chips) % chips
        at = pl.ds(pl.multiple_of(block * rows, 8), rows)
        ring_copy(k, s).wait_recv()
        spectra[k, at, :] = spectra[k, at, :] + arrived[k, s]

    def ring_step(n, carry):
        s = n // SUBS
        k = n % SUBS
        take(k, s)
        ring_copy(k, s + 1).start()
        return carry

    lax.fori_loop(0, (chips - 2) * SUBS, ring_step, 0)

    def z_copy(g, d):
        to = (fg + d) % groups
        fs = pl.ds(pl.multiple_of(g * 8, 8), 8)
        return pltpu.make_async_remote_copy(
            src_ref=sent.at[pl.ds(2 * to, 2), fs, :], dst_ref=mine.at[fg, :, fs, :],
            send_sem=z_send.at[g, d], recv_sem=z_recv.at[g, d],
            device_id=(to, p), device_id_type=MESH,
        )

    def z_landing(g, d):
        fs = pl.ds(pl.multiple_of(g * 8, 8), 8)
        return pltpu.make_async_remote_copy(
            src_ref=sent.at[pl.ds(0, 2), fs, :], dst_ref=mine.at[(fg + groups - d) % groups, :, fs, :],
            send_sem=z_send.at[g, d], recv_sem=z_recv.at[g, d],
            device_id=((fg + d) % groups, p), device_id_type=MESH,
        )

    pack = 8 // per

    def finish(g, carry):
        for i in range(pack):
            take(g * pack + i, chips - 2)
        for t in range(rows // 8):
            at = pl.ds(pl.multiple_of(z * rows + t * 8, 8), 8)
            pieces = [
                spectra[g * pack + i, at, f * half:(f + 1) * half] for i in range(pack) for f in range(per)
            ]
            turned = jnp.swapaxes(jnp.stack(pieces, 0), 0, 1)
            sent[t * 8:t * 8 + 8, pl.ds(pl.multiple_of(g * 8, 8), 8), :] = turned

        def z_start(d, carry):
            z_copy(g, far_first(d, groups)).start()
            return carry

        lax.fori_loop(1, groups, z_start, 0, unroll=UNROLL)
        fs = pl.ds(pl.multiple_of(g * 8, 8), 8)
        mine[fg, :, fs, :] = sent[pl.ds(2 * fg, 2), fs, :]
        return carry

    lax.fori_loop(0, frames // 8, finish, 0)

    def swap_copy(g):
        fs = pl.ds(pl.multiple_of(g * 8, 8), 8)
        return pltpu.make_async_remote_copy(
            src_ref=mine.at[:, :, fs, :], dst_ref=theirs.at[:, :, fs, :],
            send_sem=swap_send.at[g], recv_sem=swap_recv.at[g],
            device_id=(fg, 2 * z + 1 - core), device_id_type=MESH,
        )

    scale = 1.0 / math.sqrt(groups * frames)

    def pieces_of(ref, g):
        fs = pl.ds(pl.multiple_of(g * 8, 8), 8)
        real = halves(ref[:, 0, fs, :].reshape(groups * 8, half))
        imag = halves(ref[:, 1, fs, :].reshape(groups * 8, half))
        return real, imag

    def product(g, ref):
        real, imag = pieces_of(mine, g)
        left = [
            jnp.concatenate([jnp.concatenate([r, i], 1), jnp.concatenate([i, -r], 1)], 0)
            for r, i in zip(real, imag)
        ]
        right = [jnp.concatenate([r, i], 0) for r, i in zip(*pieces_of(ref, g))]
        return (
            (dot(left[0], right[0], TN) + dot(left[0], right[1], TN) + dot(left[1], right[0], TN)) * scale
        ).reshape(2, half, half)

    corr[...] = jnp.zeros_like(corr)

    def other_half(g):
        swap_copy(g).wait_recv()
        corr[1 - core] = corr[1 - core] + product(g, theirs)

    def ring_done(n, carry):
        ring_copy(n % SUBS, n // SUBS).wait_send()
        return carry

    lax.fori_loop(0, (chips - 1) * SUBS, ring_done, 0)

    def correlate(g, carry):
        def z_wait(d, carry):
            z_landing(g, d).wait_recv()
            return carry

        lax.fori_loop(1, groups, z_wait, 0, unroll=UNROLL)
        swap_copy(g).start()
        corr[core] = corr[core] + product(g, mine)

        @pl.when(g > 0)
        def _():
            other_half(g - 1)

        return carry

    lax.fori_loop(0, frames // 8, correlate, 0)
    other_half(frames // 8 - 1)

    block = NQ // groups
    blocks = groups // 2
    owner_core = fg // blocks

    def out_copy(i):
        return pltpu.make_async_remote_copy(
            src_ref=corr.at[:, :, pl.ds(pl.multiple_of(i * block, 8), block), :], dst_ref=landed.at[fg % blocks],
            send_sem=out_send.at[i], recv_sem=out_recv.at[fg % blocks],
            device_id=(core * blocks + i, 2 * z + owner_core), device_id_type=MESH,
        )

    def out_landing(n):
        return pltpu.make_async_remote_copy(
            src_ref=corr.at[:, :, pl.ds(0, block), :], dst_ref=landed.at[n],
            send_sem=out_send.at[n], recv_sem=out_recv.at[n],
            device_id=(core * blocks + n, 2 * z + owner_core), device_id_type=MESH,
        )

    def out_start(i, carry):
        @pl.when(core * blocks + i != fg)
        def _():
            out_copy(i).start()

        return carry

    lax.fori_loop(0, blocks, out_start, 0)

    for g in range(frames // 8):
        swap_copy(g).wait_send()

    def z_done(n, carry):
        z_copy(n // (groups - 1), 1 + n % (groups - 1)).wait_send()
        return carry

    lax.fori_loop(0, frames // 8 * (groups - 1), z_done, 0)

    @pl.when(owner_core == core)
    def _():
        i = fg % blocks
        keep = pltpu.make_async_copy(
            corr.at[:, :, pl.ds(pl.multiple_of(i * block, 8), block), :], landed.at[i], self_sem
        )
        keep.start()
        keep.wait()

    def out_wait(n, carry):
        @pl.when(core * blocks + n != fg)
        def _():
            out_landing(n).wait_recv()
            out_copy(n).wait_send()

        return carry

    lax.fori_loop(0, blocks, out_wait, 0)
    out_ref[...] = landed[...]


def linked(cake, counts, chips, groups):
    frames = cake.shape[1]
    devices = 2 * chips
    half = NQ // 2
    part = half // PARTS
    per = frames // SUBS
    rows = 2 * NH // chips
    block = NQ // groups
    blocks = groups // 2
    high, low = fourier_table()
    f32, bf = jnp.float32, jnp.bfloat16
    dma = pltpu.SemaphoreType.DMA
    away = pl.BlockSpec(memory_space=pltpu.HBM)
    vmem = pl.BlockSpec(memory_space=pltpu.VMEM)
    return pl.pallas_call(
        lambda *refs: link_kernel(chips, groups, *refs),
        out_shape=jax.ShapeDtypeStruct((blocks, 2, 2, block, half), f32),
        in_specs=[vmem, vmem, away, away],
        out_specs=vmem,
        scratch_shapes=[
            pltpu.VMEM((2 * NH, NCHI), bf),
            pltpu.VMEM((2 * NH, NCHI), bf),
            pltpu.VMEM((half, frames, NCHI), f32),
            pltpu.VMEM((frames, half, NCHI), f32),
            pltpu.VMEM((SUBS, 2 * NH, per * half), f32),
            pltpu.VMEM((SUBS, chips - 1, rows, per * half), f32),
            pltpu.VMEM((devices, 8, NCHI), f32),
            pltpu.VMEM((half, NCHI), f32),
            pltpu.VMEM((half, NCHI), f32),
            pltpu.VMEM((rows, frames, half), f32),
            pltpu.VMEM((groups, 2, frames, half), f32),
            pltpu.VMEM((groups, 2, frames, half), f32),
            pltpu.VMEM((2, 2, half, half), f32),
            pltpu.VMEM((blocks, 2, 2, block, half), f32),
            dma((2,)), dma((PARTS,)), dma((PARTS,)),
            dma((devices,)), dma((devices,)), dma((groups,)), dma((groups,)),
            dma((SUBS, chips - 1)), dma((SUBS, chips - 1)),
            dma((frames // 8, groups)), dma((frames // 8, groups)),
            dma((frames // 8,)), dma((frames // 8,)), dma((blocks,)), dma((blocks,)), dma(()),
        ],
        compiler_params=pltpu.CompilerParams(
            collective_id=0, has_side_effects=True, vmem_limit_bytes=LINK_VMEM
        ),
        name="links",
    )(cake, counts, stay(jnp.asarray(high)), stay(jnp.asarray(low)))


def fourier_table():
    harmonic = np.arange(NH)[:, None]
    phases = (harmonic * np.arange(NCHI)[None, :] % NCHI) * (2.0 * math.pi / NCHI)
    table = np.stack([np.cos(phases), -np.sin(phases)], 1) / math.sqrt(NCHI)
    table = table.reshape(2 * NH, NCHI).astype(np.float32)
    high = table.astype(jnp.bfloat16)
    return high, (table - high.astype(np.float32)).astype(jnp.bfloat16)


def solution(mesh):
    groups = mesh.shape["frames"]
    chips = mesh.shape["pix"] // 2

    def body(intensity, chi_bin, split, mask, tile_row):
        cake, counts = binned(intensity, chi_bin, split, mask, tile_row)
        blocks = linked(cake, counts, chips, groups)
        n, h, c, q, r = blocks.shape
        return blocks.transpose(3, 2, 0, 1, 4).reshape(q, c, n, h * r)

    in_specs = (P("frames", "pix"), P("pix"), P("pix"), P("pix"), P("pix"))
    out_specs = P("frames", None, "pix", None)
    return jax.shard_map(body, mesh=mesh, in_specs=in_specs, out_specs=out_specs, check_vma=False)
```
